32 devices in a mesh: dp: 8 (over z, y), tensor: 4 (over x, core).
Axes of the slice: x: 2, y: 2, z: 4, core: 2. Of those that a mesh axis runs over, the one named last changes fastest.
Arguments:
- hidden_in: bfloat16 [8, 1024, 1536], P('dp', 'tensor'), may hold values from -6 to 6
- d_out: bfloat16 [8, 1024, 1536], P('dp', 'tensor'), may hold values from -6 to 6
- in_gain: bfloat16 [1536], P('dp'), may hold values from 0.5 to 1.5
- w_zx: bfloat16 [1536, 2, 3072], P('dp', None, 'tensor'), may hold values from -0.15625 to 0.15625
- w_dt: bfloat16 [1536, 48], P('dp', 'tensor'), may hold values from -0.15625 to 0.15625
- w_bc: bfloat16 [1536, 256], P('dp'), may hold values from -0.15625 to 0.15625
- w_out: bfloat16 [1536, 3072], P('dp', 'tensor'), may hold values from -0.109375 to 0.109375
- conv_x_w: float32 [4, 3072], P(None, 'tensor'), may hold values from -0.5 to 0.5
- conv_x_b: float32 [3072], P('tensor'), may hold values from -0.5 to 0.5
- conv_bc_w: float32 [4, 256], replicated, may hold values from -0.5 to 0.5
- conv_bc_b: float32 [256], replicated, may hold values from -0.5 to 0.5
- dt_bias: float32 [48], P('tensor'), may hold values from -4.6 to -2.3
- a_log: float32 [48], P('tensor'), may hold values from 0 to 2.77
- d_skip: float32 [48], P('tensor'), may hold values from 0.5 to 1.5
- norm_scale: float32 [3072], P('tensor'), may hold values from 0.5 to 1.5
Outputs:
- block_out: bfloat16 [8, 1024, 1536], P('dp', 'tensor')
- d_hidden: float32 [8, 1024, 1536], P('dp', 'tensor')
- g_in_gain: float32 [1536], P('dp')
- g_w_zx: float32 [1536, 2, 3072], P('dp', None, 'tensor')
- g_w_dt: float32 [1536, 48], P('dp', 'tensor')
- input_output_weight_grad: float32 [1536, 256], P('dp')
- g_w_out: float32 [1536, 3072], P('dp', 'tensor')
- g_conv_x_w: float32 [4, 3072], P(None, 'tensor')
- g_conv_x_b: float32 [3072], P('tensor')
- g_conv_bc_w: float32 [4, 256], replicated
- g_conv_bc_b: float32 [256], replicated
- g_dt_bias: float32 [48], P('tensor')
- g_a_log: float32 [48], P('tensor')
- g_d_skip: float32 [48], P('tensor')
- g_norm_scale: float32 [3072], P('tensor')
The draws below stay inside these ranges and needn't reach their ends.
All inputs are finite; a program needn't handle non-finite values.
Results may differ from the reference program's by a relative error of at most 0.0085.
Values may be sent and summed in bfloat16 or wider, within the bound.
A program may use at most 192 MiB of HBM per device.

```python
import jax
import jax.numpy as jnp
from jax import lax

D = 1536
HEADS = 48
STATE = 128
CONV = 4
SPAN = 256
SEQ_LEN = 1024
SEQ_DEV = 1
INNER = 3072
SEQS = 8
N_DP = 8


def levels(key, shape, shards, smallest, largest):
    loudness = 1.0
    for dim, parts in shards:
        steps = jax.random.uniform(jax.random.fold_in(jax.random.fold_in(key, 6), dim), (parts,), jnp.float32, smallest / len(shards), largest / len(shards))
        loudness = loudness * jnp.repeat(jnp.exp(steps), shape[dim] // parts).reshape((-1,) + (1,) * (len(shape) - 1 - dim))
    return loudness


def normal_values(stream_key, extent, deviation, most, cuts=(), held_as=jnp.bfloat16):
    level = levels(stream_key, extent, cuts, -0.22, 0.18) if cuts else 1.0
    values = jax.random.normal(stream_key, extent, jnp.float32) * deviation * level
    return jnp.minimum(jnp.maximum(values, -most), most).astype(held_as)


def setup_inputs(seed: int = 0) -> dict:
    keys = jax.random.split(jax.random.key(seed), 16)
    hidden_in = normal_values(keys[0], (SEQS, SEQ_LEN, D), 1.0, 6.0, ((0, 8), (1, 4)))
    d_out = normal_values(keys[1], (SEQS, SEQ_LEN, D), 1.0, 6.0, ((0, 8), (1, 4)))
    in_gain = jnp.clip(1.0 + 0.1 * jax.random.normal(keys[2], (D,), jnp.float32), 0.5, 1.5).astype(jnp.bfloat16)
    w_zx = normal_values(keys[3], (D, 2, INNER), D ** -0.5, 0.15625, ((0, 8), (2, 4)))
    w_dt = normal_values(keys[4], (D, HEADS), D ** -0.5, 0.15625, ((0, 8), (1, 4)))
    w_bc = normal_values(keys[5], (D, 2 * STATE), D ** -0.5, 0.15625, ((0, 8),))
    w_out = normal_values(keys[6], (D, INNER), INNER ** -0.5, 0.109375, ((0, 8), (1, 4)))
    conv_x_w = jnp.clip(jax.random.uniform(keys[7], (CONV, INNER), jnp.float32, -0.5, 0.5) * levels(keys[7], (CONV, INNER), ((1, 4),), -0.4, 0.0), -0.5, 0.5)
    conv_x_b = jnp.clip(jax.random.uniform(keys[8], (INNER,), jnp.float32, -0.5, 0.5) * levels(keys[8], (INNER,), ((0, 4),), -0.4, 0.0), -0.5, 0.5)
    conv_bc_w = jnp.clip(jax.random.uniform(keys[9], (CONV, 2 * STATE), jnp.float32, -0.5, 0.5), -0.5, 0.5)
    conv_bc_b = jnp.clip(jax.random.uniform(keys[10], (2 * STATE,), jnp.float32, -0.5, 0.5), -0.5, 0.5)
    dt_bias = jnp.clip(-4.6 + 2.3 * jax.random.uniform(keys[11], (HEADS,), jnp.float32) ** levels(keys[11], (HEADS,), ((0, 4),), -0.2, 0.2), -4.6, -2.3)
    a_log = jnp.clip(2.77 * jax.random.uniform(keys[12], (HEADS,), jnp.float32) ** levels(keys[12], (HEADS,), ((0, 4),), -0.2, 0.2), 0.0, 2.77)
    d_skip = jnp.clip(0.5 + 1.0 * jax.random.uniform(keys[13], (HEADS,), jnp.float32) ** levels(keys[13], (HEADS,), ((0, 4),), -0.2, 0.2), 0.5, 1.5)
    norm_scale = jnp.clip(1.0 + 0.1 * jax.random.normal(keys[14], (INNER,), jnp.float32), 0.5, 1.5)
    return dict(hidden_in=hidden_in, d_out=d_out, in_gain=in_gain, w_zx=w_zx, w_dt=w_dt, w_bc=w_bc, w_out=w_out, conv_x_w=conv_x_w, conv_x_b=conv_x_b, conv_bc_w=conv_bc_w, conv_bc_b=conv_bc_b, dt_bias=dt_bias, a_log=a_log, d_skip=d_skip, norm_scale=norm_scale)


EPSILON = 1e-05
HIGHEST = lax.Precision.HIGHEST

@jax.custom_vjp
def low(v):
    return lax.optimization_barrier(v.astype(jnp.bfloat16)).astype(jnp.float32)

@jax.custom_vjp
def low_back(v):
    return v

def low_keep(v):
    return (low(v), None)

def low_pass(kept, grad):
    return (grad,)

def back_keep(v):
    return (v, None)

def back_low(kept, grad):
    return (low(grad),)
low.defvjp(low_keep, low_pass)
low_back.defvjp(back_keep, back_low)

def causal_conv(inputs, kernel, conv_bias):
    kernel_taps = kernel.shape[0]
    seq_len = inputs.shape[1]
    padded = jnp.pad(inputs, ((0, 0), (kernel_taps - 1, 0), (0, 0)))
    result = conv_bias + kernel[0] * padded[:, 0:seq_len]
    for offset in range(1, kernel_taps):
        result = result + kernel[offset] * padded[:, offset:offset + seq_len]
    return result

def span_scan(values, timestep_widths, decay_rate, in_map, out_map):
    batch_seqs, seq_len, head_count, head_width = values.shape
    state_dim = in_map.shape[-1]
    blocks = seq_len // SPAN
    scaled_x = (values * timestep_widths[..., None]).reshape(batch_seqs, blocks, SPAN, head_count, head_width)
    decay_log = (timestep_widths * decay_rate).reshape(batch_seqs, blocks, SPAN, head_count)
    cumulative = jnp.cumsum(decay_log, axis=2)
    cumulative_h = jnp.moveaxis(cumulative, 3, 2)
    in_blocks = in_map.reshape(batch_seqs, blocks, SPAN, state_dim)
    out_blocks = out_map.reshape(batch_seqs, blocks, SPAN, state_dim)
    position = jnp.arange(SPAN)
    causal = position[:, None] >= position[None, :]
    log_gap = cumulative_h[..., :, None] - cumulative_h[..., None, :]
    within = jnp.where(causal, jnp.exp(jnp.where(causal, log_gap, 0.0)), 0.0)
    scores = jnp.einsum('scin,scjn->scij', out_blocks, in_blocks, precision=HIGHEST)
    mixed_weights = within * scores[:, :, None]
    diag_part = jnp.einsum('schij,scjhp->scihp', mixed_weights, scaled_x, precision=HIGHEST)
    last_step = cumulative_h[..., -1]
    to_end = jnp.exp(last_step[..., None] - cumulative_h)
    weighted = scaled_x * jnp.moveaxis(to_end, 2, 3)[..., None]
    block_states = jnp.einsum('scjhp,scjn->schpn', weighted, in_blocks, precision=HIGHEST)
    carried_state = jnp.zeros((batch_seqs, head_count, head_width, state_dim), jnp.float32)
    entering = []
    for block_index in range(blocks):
        entering.append(carried_state)
        carried_state = jnp.exp(last_step[:, block_index])[..., None, None] * carried_state + block_states[:, block_index]
    start_states = jnp.stack(entering, axis=1)
    carry_part = jnp.einsum('scin,schpn->scihp', out_blocks, start_states, precision=HIGHEST) * jnp.exp(cumulative)[..., None]
    return (diag_part + carry_part).reshape(batch_seqs, seq_len, head_count, head_width)

def mixer(gate_in, inner_in, delta_in, bc_proj, conv_x_w, conv_x_b, conv_bc_w, conv_bc_b, dt_bias, a_log, d_skip):
    x_conv = jax.nn.silu(causal_conv(inner_in, conv_x_w, conv_x_b))
    bc_conv = jax.nn.silu(causal_conv(bc_proj, conv_bc_w, conv_bc_b))
    state_dim = bc_conv.shape[-1] // 2
    timestep_widths = jax.nn.softplus(delta_in + dt_bias)
    decay_rate = -jnp.exp(a_log)
    batch_seqs, seq_len, channels = x_conv.shape
    head_count = timestep_widths.shape[-1]
    values = x_conv.reshape(batch_seqs, seq_len, head_count, channels // head_count)
    ssd_out = span_scan(values, timestep_widths, decay_rate, bc_conv[..., :state_dim], bc_conv[..., state_dim:])
    ssd_out = ssd_out + d_skip[:, None] * values
    return ssd_out.reshape(batch_seqs, seq_len, channels) * jax.nn.silu(gate_in)

def in_rmsnorm(hidden, gain_vec):
    return hidden * lax.rsqrt(lax.optimization_barrier(jnp.mean(hidden * hidden, axis=-1, keepdims=True)) + EPSILON) * gain_vec

def block_forward(hidden, params):
    gain_vec, w_zx, w_dt, w_bc, w_out, conv_x_w, conv_x_b, conv_bc_w, conv_bc_b, dt_bias, a_log, d_skip, norm_scale = params
    batch_seqs, seq_len, model_width = hidden.shape
    inner_width = w_zx.shape[2]
    normed = low(in_rmsnorm(hidden, gain_vec)).reshape(-1, model_width)
    both_proj = jnp.dot(normed, w_zx.reshape(model_width, 2 * inner_width), precision=HIGHEST)
    gate_in = low_back(both_proj[:, :inner_width]).reshape(batch_seqs, seq_len, inner_width)
    inner_in = low_back(both_proj[:, inner_width:]).reshape(batch_seqs, seq_len, inner_width)
    delta_in = low_back(jnp.dot(normed, w_dt, precision=HIGHEST)).reshape(batch_seqs, seq_len, -1)
    bc_proj = low_back(jnp.dot(normed, w_bc, precision=HIGHEST)).reshape(batch_seqs, seq_len, -1)
    gated_y = mixer(gate_in, inner_in, delta_in, bc_proj, conv_x_w, conv_x_b, conv_bc_w, conv_bc_b, dt_bias, a_log, d_skip)
    normed_y = low(gated_y * lax.rsqrt(lax.optimization_barrier(jnp.mean(gated_y * gated_y, axis=-1, keepdims=True)) + EPSILON) * norm_scale)
    branch = jnp.dot(normed_y.reshape(-1, inner_width), w_out.T, precision=HIGHEST)
    return hidden + branch.reshape(batch_seqs, seq_len, model_width)

def reference(hidden_in, d_out, in_gain, w_zx, w_dt, w_bc, w_out, conv_x_w, conv_x_b, conv_bc_w, conv_bc_b, dt_bias, a_log, d_skip, norm_scale):
    params = tuple((member.astype(jnp.float32) for member in (in_gain, w_zx, w_dt, w_bc, w_out, conv_x_w, conv_x_b, conv_bc_w, conv_bc_b, dt_bias, a_log, d_skip, norm_scale)))
    hidden = hidden_in.astype(jnp.float32)

    def whole(hidden_all, weights):
        groups = hidden_all.reshape(N_DP, SEQ_DEV, SEQ_LEN, D)

        def scan_step(carry, group):
            return (carry, block_forward(group, weights))
        checked = jax.checkpoint(scan_step)
        final, outputs = lax.scan(checked, jnp.zeros((), jnp.float32), groups)
        return outputs.reshape(SEQS, SEQ_LEN, D)
    result, pullback = jax.vjp(whole, hidden, params)
    d_hidden, d_params = pullback(d_out.astype(jnp.float32))
    return (result.astype(jnp.bfloat16), d_hidden, d_params[0], d_params[1], d_params[2], d_params[3], d_params[4], d_params[5], d_params[6], d_params[7], d_params[8], d_params[9], d_params[10], d_params[11], d_params[12])
```

```python
import jax
import jax.numpy as jnp
from jax import lax
from jax.experimental import pallas as pl
from jax.experimental.pallas import tpu as pltpu
from jax.sharding import PartitionSpec as P

Q = 128
STATE = 128
WIDTH = 64
NEG = -1e30
EPSILON = 1e-05
HIGHEST = lax.Precision.HIGHEST
F32 = jnp.float32
BF16 = jnp.bfloat16


def dot(a, b, dims=((1,), (0,)), precision=None):
    return lax.dot_general(a, b, (dims, ((), ())), precision=precision, preferred_element_type=F32)


def low(v):
    return v.astype(BF16)


def tri_masks():
    row = lax.broadcasted_iota(jnp.int32, (Q, Q), 0)
    col = lax.broadcasted_iota(jnp.int32, (Q, Q), 1)
    return row, col


def conv_block(buf, taps, bias):
    out = bias + taps[0:1] * buf[pl.ds(5, Q), :]
    for k in range(1, 4):
        out = out + taps[k : k + 1] * buf[pl.ds(5 + k, Q), :]
    return out


def softplus(v):
    return jnp.maximum(v, 0.0) + jnp.log1p(jnp.exp(-jnp.abs(v)))


def spread(columns, pair, low_half):
    first = jnp.broadcast_to(columns[:, 2 * pair : 2 * pair + 1], (columns.shape[0], 2 * WIDTH))
    second = jnp.broadcast_to(
        columns[:, 2 * pair + 1 : 2 * pair + 2], (columns.shape[0], 2 * WIDTH)
    )
    return first, second, jnp.where(low_half[: columns.shape[0]], first, second)


def forward_kernel(
    inner_ref, small_ref, xw_ref, xb_ref, bcw_ref, bcb_ref, bias_ref, alog_ref, skip_ref,
    y_ref, state_out_ref, xbuf, bcbuf, state, mixed, weighted,
):
    step = pl.program_id(0)
    heads = bias_ref.shape[1]

    @pl.when(step == 0)
    def _():
        state[...] = jnp.zeros_like(state)
        xbuf[0:8, :] = jnp.zeros((8, xbuf.shape[1]), F32)
        bcbuf[0:8, :] = jnp.zeros((8, bcbuf.shape[1]), F32)

    xbuf[8:, :] = inner_ref[...]
    bcbuf[8:, :] = small_ref[:, : 2 * STATE]
    row, col = tri_masks()
    causal = row >= col
    low_half = col < WIDTH
    pre_bc = conv_block(bcbuf, bcw_ref[...], bcb_ref[...])
    bc = low(pre_bc * jax.nn.sigmoid(pre_bc))
    b, c = bc[:, :STATE], bc[:, STATE:]
    dt = softplus(small_ref[:, 2 * STATE :] + bias_ref[...])
    decay = dt * -jnp.exp(alog_ref[...])
    cum = dot(causal.astype(F32), decay, precision=HIGHEST)
    cum_t = cum.T
    scores = dot(c, b, ((1,), (1,)))
    state_low = low(state[...])
    state_out_ref[0] = state[...]
    carried = dot(c, state_low)
    xw, xb = xw_ref[...], xb_ref[...]
    skip = skip_ref[...]
    for pair in range(heads // 2):
        sl = slice(2 * WIDTH * pair, 2 * WIDTH * (pair + 1))
        pre = xb[:, sl] + xw[0:1, sl] * xbuf[pl.ds(5, Q), sl]
        for k in range(1, 4):
            pre = pre + xw[k : k + 1, sl] * xbuf[pl.ds(5 + k, Q), sl]
        x = pre * jax.nn.sigmoid(pre)
        _, _, dt_e = spread(dt, pair, low_half)
        _, _, skip_e = spread(skip, pair, low_half)
        cum_0, cum_1, cum_e = spread(cum, pair, low_half)
        xh = x * dt_e
        parts = []
        for h, cum_h in ((2 * pair, cum_0), (2 * pair + 1, cum_1)):
            gap = cum_h - cum_t[h : h + 1, :]
            parts.append(low(jnp.exp(jnp.where(causal, gap, NEG)) * scores))
        xl = low(xh)
        zero = jnp.zeros_like(xl)
        stacked = jnp.concatenate([jnp.where(low_half, xl, zero), jnp.where(low_half, zero, xl)], 0)
        y = dot(jnp.concatenate(parts, 1), stacked)
        last = cum_e[Q - 1 : Q, :]
        y = y + carried[:, sl] * jnp.exp(cum_e) + skip_e * x
        y_ref[:, sl] = y
        weighted[:, sl] = low(xh * jnp.exp(last - cum_e))
        mixed[:, sl] = jnp.exp(last)
    state[...] = state[...] * mixed[...] + dot(b.T, weighted[...])
    xbuf[0:8, :] = xbuf[Q : Q + 8, :]
    bcbuf[0:8, :] = bcbuf[Q : Q + 8, :]


def full(shape):
    return pl.BlockSpec(shape, lambda i: (0,) * len(shape))


def mixer_forward(inner, small, xw, xb, bcw, bcb, bias, alog, skip):
    rows, channels = inner.shape
    blocks = rows // Q
    wide = small.shape[1]
    return pl.pallas_call(
        forward_kernel,
        name="mixer_forward",
        grid=(blocks,),
        in_specs=[
            pl.BlockSpec((Q, channels), lambda i: (i, 0)),
            pl.BlockSpec((Q, wide), lambda i: (i, 0)),
            full(xw.shape), full(xb.shape), full(bcw.shape), full(bcb.shape),
            full(bias.shape), full(alog.shape), full(skip.shape),
        ],
        out_specs=[
            pl.BlockSpec((Q, channels), lambda i: (i, 0)),
            pl.BlockSpec((1, STATE, channels), lambda i: (i, 0, 0)),
        ],
        out_shape=[
            jax.ShapeDtypeStruct((rows, channels), F32),
            jax.ShapeDtypeStruct((blocks, STATE, channels), F32),
        ],
        scratch_shapes=[
            pltpu.VMEM((Q + 8, channels), F32),
            pltpu.VMEM((Q + 8, 2 * STATE), F32),
            pltpu.VMEM((STATE, channels), F32),
            pltpu.VMEM((1, channels), F32),
            pltpu.VMEM((Q, channels), BF16),
        ],
        cost_estimate=pl.CostEstimate(
            flops=rows * channels * Q * 8, bytes_accessed=rows * channels * 16, transcendentals=rows * channels * 8
        ),
    )(inner, small, xw, xb, bcw, bcb, bias, alog, skip)


def backward_kernel(
    inner_ref, prev_ref, small_ref, sprev_ref, gy_ref, state_ref,
    xw_ref, xb_ref, bcw_ref, bcb_ref, bias_ref, alog_ref, skip_ref,
    dinner_ref, ddt_ref, dbc_ref, gxw_ref, gbcw_ref, ghead_ref,
    xbuf, bcbuf, dxbuf, dbcbuf, dstate, carried, back, rows_buf, sums, cgy, weighted, decay_row,
):
    step = pl.program_id(0)
    blocks = pl.num_programs(0)
    heads = bias_ref.shape[1]
    channels = inner_ref.shape[1]

    @pl.when(step == 0)
    def _():
        dstate[...] = jnp.zeros_like(dstate)
        dxbuf[Q:, :] = jnp.zeros((8, channels), F32)
        dbcbuf[Q:, :] = jnp.zeros((8, 2 * STATE), F32)
        gxw_ref[...] = jnp.zeros_like(gxw_ref)
        gbcw_ref[...] = jnp.zeros_like(gbcw_ref)
        ghead_ref[...] = jnp.zeros_like(ghead_ref)

    first = step == blocks - 1
    xbuf[0:8, :] = jnp.where(first, 0.0, prev_ref[...])
    bcbuf[0:8, :] = jnp.where(first, 0.0, sprev_ref[:, : 2 * STATE])
    xbuf[8:, :] = inner_ref[...]
    bcbuf[8:, :] = small_ref[:, : 2 * STATE]
    row, col = tri_masks()
    causal = row >= col
    causal_t = col >= row
    low_half = col < WIDTH
    pre_bc = conv_block(bcbuf, bcw_ref[...], bcb_ref[...])
    sig_bc = jax.nn.sigmoid(pre_bc)
    bc = low(pre_bc * sig_bc)
    b, c = bc[:, :STATE], bc[:, STATE:]
    raw = small_ref[:, 2 * STATE :] + bias_ref[...]
    dt = softplus(raw)
    a = -jnp.exp(alog_ref[...])
    cum = dot(causal.astype(F32), dt * a, precision=HIGHEST)
    cum_t = cum.T
    scores_t = dot(b, c, ((1,), (1,)))
    dstate_low = low(dstate[...])
    state_low = low(state_ref[0])
    carried[...] = dot(c, state_low)
    back[...] = dot(b, dstate_low)
    xw, xb = xw_ref[...], xb_ref[...]
    skip = skip_ref[...]
    dscores_t = jnp.zeros((Q, Q), F32)
    cols = jnp.zeros((Q, heads), F32)
    hot_row = lax.broadcasted_iota(jnp.int32, (2 * Q, heads), 0) // Q
    hot_col = lax.broadcasted_iota(jnp.int32, (2 * Q, heads), 1)
    for pair in range(heads // 2):
        sl = slice(2 * WIDTH * pair, 2 * WIDTH * (pair + 1))
        shifted = [xbuf[pl.ds(5 + k, Q), sl] for k in range(4)]
        pre = xb[:, sl] + xw[0:1, sl] * shifted[0]
        for k in range(1, 4):
            pre = pre + xw[k : k + 1, sl] * shifted[k]
        sig = jax.nn.sigmoid(pre)
        x = pre * sig
        _, _, dt_e = spread(dt, pair, low_half)
        _, _, skip_e = spread(skip, pair, low_half)
        cum_0, cum_1, cum_e = spread(cum, pair, low_half)
        last = cum_e[Q - 1 : Q, :]
        xh = x * dt_e
        xl = low(xh)
        gy = gy_ref[:, sl]
        gl = low(gy)
        zero = jnp.zeros_like(gl)
        g_stack = jnp.concatenate([jnp.where(low_half, gl, zero), jnp.where(low_half, zero, gl)], 0)
        dmixed_t = dot(xl, g_stack, ((1,), (1,)))
        mixes, zs = [], []
        for i, (h, cum_h) in enumerate(((2 * pair, cum_0), (2 * pair + 1, cum_1))):
            gap = cum_t[h : h + 1, :] - cum_h
            within = jnp.exp(jnp.where(causal_t, gap, NEG))
            mix = within * scores_t
            dm = dmixed_t[:, i * Q : (i + 1) * Q]
            dscores_t = dscores_t + dm * within
            z = low(dm * mix)
            zs.append(z)
            mixes.append(low(mix))
            rows_buf[h : h + 1, :] = jnp.sum(z.astype(F32), axis=0, keepdims=True)
        hot = (hot_col == hot_row + 2 * pair).astype(BF16)
        cols = cols + dot(jnp.concatenate(zs, 1), hot)
        dxh = dot(jnp.concatenate(mixes, 1), g_stack)
        to_end = jnp.exp(last - cum_e)
        from_state = to_end * back[:, sl]
        dxh = dxh + from_state
        grown = jnp.exp(cum_e) * gy
        cgy[:, sl] = low(grown)
        weighted[:, sl] = low(xh * to_end)
        sums[0:Q, sl] = low(grown * carried[:, sl])
        sums[Q : 2 * Q, sl] = low(xh * from_state)
        sums[2 * Q : 3 * Q, sl] = low(dxh * x)
        sums[3 * Q : 4 * Q, sl] = low(gy * x)
        decay_row[:, sl] = jnp.exp(last)
        dx = dxh * dt_e + skip_e * gy
        dpre = dx * (sig * (1.0 + pre * (1.0 - sig)))
        dxbuf[0:Q, sl] = dpre
        out = xw[3:4, sl] * dpre
        for k in range(3):
            out = out + xw[k : k + 1, sl] * dxbuf[pl.ds(3 - k, Q), sl]
        dinner_ref[:, sl] = low(out)
        for k in range(4):
            gxw_ref[k : k + 1, sl] += jnp.sum(dpre * shifted[k], axis=0, keepdims=True)
        gxw_ref[4:5, sl] += jnp.sum(dpre, axis=0, keepdims=True)
    head_of = lax.broadcasted_iota(jnp.int32, (channels, heads), 0) // WIDTH
    head = lax.broadcasted_iota(jnp.int32, (channels, heads), 1)
    head_hot = (head_of == head).astype(BF16)
    head_sums = dot(sums[...], head_hot)
    v, u = head_sums[0:Q], head_sums[Q : 2 * Q]
    t_x, t_skip = head_sums[2 * Q : 3 * Q], head_sums[3 * Q :]
    kept = jnp.sum(dstate[...] * state_ref[0], axis=0, keepdims=True) * decay_row[...]
    dlast = dot(jnp.broadcast_to(kept, (8, channels)), head_hot.astype(F32), precision=HIGHEST)[0:1]
    dlast = dlast + jnp.sum(u, axis=0, keepdims=True)
    dcum = rows_buf[0:heads, :].T - cols + v - u
    ddecay = dot(causal_t.astype(F32), dcum, precision=HIGHEST) + dlast
    ddt = (ddecay * a + t_x) * jax.nn.sigmoid(raw)
    ddt_ref[...] = low(ddt)
    ghead_ref[0:1, :] += jnp.sum(ddt, axis=0, keepdims=True)
    ghead_ref[1:2, :] += jnp.sum(ddecay * dt, axis=0, keepdims=True) * a
    ghead_ref[2:3, :] += jnp.sum(t_skip, axis=0, keepdims=True)
    dsl = low(dscores_t)
    dc = dot(dsl, b, ((0,), (0,))) + dot(cgy[...], state_low, ((1,), (1,)))
    db = dot(dsl, c) + dot(weighted[...], dstate_low, ((1,), (1,)))
    dstate[...] = dstate[...] * decay_row[...] + dot(c.T, cgy[...])
    dbc = jnp.concatenate([db, dc], 1)
    dpre = dbc * (sig_bc * (1.0 + pre_bc * (1.0 - sig_bc)))
    dbcbuf[0:Q, :] = dpre
    bcw = bcw_ref[...]
    out = bcw[3:4] * dpre
    for k in range(3):
        out = out + bcw[k : k + 1] * dbcbuf[pl.ds(3 - k, Q), :]
    dbc_ref[...] = out.astype(dbc_ref.dtype)
    for k in range(4):
        gbcw_ref[k : k + 1, :] += jnp.sum(dpre * bcbuf[pl.ds(5 + k, Q), :], axis=0, keepdims=True)
    gbcw_ref[4:5, :] += jnp.sum(dpre, axis=0, keepdims=True)
    dxbuf[Q:, :] = dxbuf[0:8, :]
    dbcbuf[Q:, :] = dbcbuf[0:8, :]


def mixer_backward(inner, small, gy, states, xw, xb, bcw, bcb, bias, alog, skip, dbc_dtype=F32):
    rows, channels = inner.shape
    blocks = rows // Q
    wide = small.shape[1]
    heads = bias.shape[1]
    at = lambda i: blocks - 1 - i
    before = lambda i: jnp.maximum(at(i) * (Q // 8) - 1, 0)
    return pl.pallas_call(
        backward_kernel,
        name="mixer_backward",
        grid=(blocks,),
        in_specs=[
            pl.BlockSpec((Q, channels), lambda i: (at(i), 0)),
            pl.BlockSpec((8, channels), lambda i: (before(i), 0)),
            pl.BlockSpec((Q, wide), lambda i: (at(i), 0)),
            pl.BlockSpec((8, wide), lambda i: (before(i), 0)),
            pl.BlockSpec((Q, channels), lambda i: (at(i), 0)),
            pl.BlockSpec((1, STATE, channels), lambda i: (at(i), 0, 0)),
            full(xw.shape), full(xb.shape), full(bcw.shape), full(bcb.shape),
            full(bias.shape), full(alog.shape), full(skip.shape),
        ],
        out_specs=[
            pl.BlockSpec((Q, channels), lambda i: (at(i), 0)),
            pl.BlockSpec((Q, heads), lambda i: (at(i), 0)),
            pl.BlockSpec((Q, 2 * STATE), lambda i: (at(i), 0)),
            full((5, channels)), full((5, 2 * STATE)), full((3, heads)),
        ],
        out_shape=[
            jax.ShapeDtypeStruct((rows, channels), BF16),
            jax.ShapeDtypeStruct((rows, heads), BF16),
            jax.ShapeDtypeStruct((rows, 2 * STATE), dbc_dtype),
            jax.ShapeDtypeStruct((5, channels), F32),
            jax.ShapeDtypeStruct((5, 2 * STATE), F32),
            jax.ShapeDtypeStruct((3, heads), F32),
        ],
        scratch_shapes=[
            pltpu.VMEM((Q + 8, channels), F32),
            pltpu.VMEM((Q + 8, 2 * STATE), F32),
            pltpu.VMEM((Q + 8, channels), F32),
            pltpu.VMEM((Q + 8, 2 * STATE), F32),
            pltpu.VMEM((STATE, channels), F32),
            pltpu.VMEM((Q, channels), F32),
            pltpu.VMEM((Q, channels), F32),
            pltpu.VMEM((16, Q), F32),
            pltpu.VMEM((4 * Q, channels), BF16),
            pltpu.VMEM((Q, channels), BF16),
            pltpu.VMEM((Q, channels), BF16),
            pltpu.VMEM((1, channels), F32),
        ],
        cost_estimate=pl.CostEstimate(
            flops=rows * channels * Q * 20, bytes_accessed=rows * channels * 20, transcendentals=rows * channels * 10
        ),
    )(inner, inner, small, small, gy, states, xw, xb, bcw, bcb, bias, alog, skip)


def local(
    hidden_in, d_out, in_gain, w_zx, w_dt, w_bc, w_out,
    conv_x_w, conv_x_b, conv_bc_w, conv_bc_b, dt_bias, a_log, d_skip, norm_scale,
):
    _, rows_local, width = hidden_in.shape
    inner_local = w_zx.shape[2]
    heads = w_dt.shape[1]
    tensor_index = lax.axis_index("tensor")
    parts = lax.axis_size("tensor")
    hidden_bf = lax.all_gather(hidden_in[0], "tensor", axis=0, tiled=True)
    first_pack = jnp.concatenate([w_zx[:, 1, :], w_bc, w_dt, in_gain[:, None]], 1)
    first = lax.all_gather(first_pack, "dp", axis=0, tiled=True)
    second_pack = jnp.concatenate([w_zx[:, 0, :], w_out], 1)
    second = lax.all_gather(second_pack, "dp", axis=0, tiled=True)
    dout_all = lax.all_gather(d_out[0], "tensor", axis=0, tiled=True)
    w_inner = first[:, :inner_local]
    w_small = first[:, inner_local : inner_local + 2 * STATE + heads]
    gain = first[:, -1].astype(F32)[None]
    w_gate, w_o = second[:, :inner_local], second[:, inner_local:]

    hidden = hidden_bf.astype(F32)
    rh = lax.rsqrt(jnp.mean(hidden * hidden, axis=-1, keepdims=True) + EPSILON)
    xn = low(hidden * rh * gain)
    inner = dot(xn, w_inner)
    small = dot(xn, w_small)
    params = (
        conv_x_w, conv_x_b[None], conv_bc_w, conv_bc_b[None], dt_bias[None], a_log[None], d_skip[None],
    )
    y, states = mixer_forward(inner, small, *params)
    gate = dot(xn, w_gate)
    dyn = dot(dout_all, w_o)
    sig = jax.nn.sigmoid(gate)
    act = gate * sig
    gated = y * act
    scale = norm_scale[None]
    scaled = dyn * scale
    sums = lax.psum(jnp.stack([jnp.sum(gated * gated, -1), jnp.sum(scaled * gated, -1)]), "tensor")
    channels = inner_local * parts
    r = lax.rsqrt(sums[0] / channels + EPSILON)[:, None]
    yn = low(gated * r * scale)
    d_gated = r * scaled - gated * (r * r * r) * sums[1][:, None] / channels
    g_scale = jnp.sum(dyn * gated * r, axis=0)
    gy = d_gated * act
    d_gate = low(d_gated * y * (sig * (1.0 + gate * (1.0 - sig))))
    g_out = low(dot(dout_all, yn, ((0,), (0,))))
    g_gate = low(dot(xn, d_gate, ((0,), (0,))))
    early = lax.psum_scatter(
        jnp.concatenate([g_gate, g_out], 1), "dp", scatter_dimension=0, tiled=True
    ).astype(F32)
    partial_out = low(dot(yn, w_o, ((1,), (1,))))
    branch = lax.psum_scatter(partial_out, "tensor", scatter_dimension=0, tiled=True)
    hidden_own = hidden_in[0].astype(F32)
    block_out = low(hidden_own + branch.astype(F32))

    d_inner, d_dt, d_bc, g_x, g_bc, g_head = mixer_backward(
        inner, small, gy, states, *params, dbc_dtype=BF16
    )
    d_bc_low = lax.psum(d_bc, "tensor")
    own_columns = 2 * STATE // parts
    d_bc_own = lax.dynamic_slice_in_dim(d_bc_low, tensor_index * own_columns, own_columns, 1)
    late = jnp.concatenate([d_inner, d_bc_own, d_dt], 1)
    g_late = low(dot(xn, late, ((0,), (0,))))
    late_sum = lax.psum_scatter(g_late, "dp", scatter_dimension=0, tiled=True).astype(F32)
    w_small_own = jnp.concatenate(
        [
            lax.dynamic_slice_in_dim(first, inner_local + tensor_index * own_columns, own_columns, 1),
            w_small[:, 2 * STATE :],
        ],
        1,
    )
    d_xn = dot(d_gate, w_gate, ((1,), (1,))) + dot(d_inner, w_inner, ((1,), (1,)))
    d_xn = d_xn + dot(late[:, inner_local:], w_small_own, ((1,), (1,)))
    d_normed = lax.psum_scatter(low(d_xn), "tensor", scatter_dimension=0, tiled=True).astype(F32)
    rh_own = lax.rsqrt(jnp.mean(hidden_own * hidden_own, axis=-1, keepdims=True) + EPSILON)
    weighted = d_normed * gain
    g_gain = jnp.sum(d_normed * hidden_own * rh_own, axis=0)
    inner_sum = jnp.sum(weighted * hidden_own, axis=-1, keepdims=True)
    d_hidden = (
        d_out[0].astype(F32) + rh_own * weighted - hidden_own * (rh_own * rh_own * rh_own) * inner_sum / width
    )
    flat = jnp.concatenate(
        [g_gain, g_bc.reshape(-1), g_x.reshape(-1), g_scale, g_head.reshape(-1)]
    )
    flat = lax.psum(flat, "dp")
    shared_size = width + 5 * 2 * STATE
    shared = lax.psum(flat[:shared_size], "tensor")
    own = lax.dynamic_slice_in_dim(shared, lax.axis_index("dp") * in_gain.shape[0], in_gain.shape[0], 0)
    g_bc = shared[width:].reshape(5, 2 * STATE)
    g_x = flat[shared_size : shared_size + 5 * inner_local].reshape(5, inner_local)
    rest = flat[shared_size + 5 * inner_local :]
    g_scale = rest[:inner_local]
    g_head = rest[inner_local:].reshape(3, heads)
    g_w_bc = lax.all_gather(late_sum[:, inner_local : inner_local + own_columns], "tensor", axis=1, tiled=True)
    g_zx = jnp.stack([early[:, :inner_local], late_sum[:, :inner_local]], 1)
    return (
        block_out[None],
        d_hidden[None],
        own,
        g_zx,
        late_sum[:, inner_local + own_columns :],
        g_w_bc,
        early[:, inner_local:],
        g_x[:4],
        g_x[4],
        g_bc[:4],
        g_bc[4],
        g_head[0],
        g_head[1],
        g_head[2],
        g_scale,
    )


def solution(mesh):
    tokens = P("dp", "tensor", None)
    specs = (
        tokens,
        tokens,
        P("dp"),
        P("dp", None, "tensor"),
        P("dp", "tensor"),
        P("dp", None),
        P("dp", "tensor"),
        P(None, "tensor"),
        P("tensor"),
        P(),
        P(),
        P("tensor"),
        P("tensor"),
        P("tensor"),
        P("tensor"),
    )
    return jax.shard_map(local, mesh=mesh, in_specs=specs, out_specs=specs, check_vma=False)
```

```python
import jax
import jax.numpy as jnp
from jax import lax
from jax.experimental import pallas as pl
from jax.experimental.pallas import tpu as pltpu
from jax.sharding import PartitionSpec as P

Q = 128
STATE = 128
WIDTH = 64
NEG = -1e30
EPSILON = 1e-05
MESH = pl.DeviceIdType.MESH
HIGHEST = lax.Precision.HIGHEST
F32 = jnp.float32
BF16 = jnp.bfloat16


def dot(a, b, dims=((1,), (0,)), precision=None):
    return lax.dot_general(a, b, (dims, ((), ())), precision=precision, preferred_element_type=F32)


def low(v):
    return v.astype(BF16)


def tri_masks():
    row = lax.broadcasted_iota(jnp.int32, (Q, Q), 0)
    col = lax.broadcasted_iota(jnp.int32, (Q, Q), 1)
    return row, col


def conv_block(buf, taps, bias):
    out = bias + taps[0:1] * buf[pl.ds(5, Q), :]
    for k in range(1, 4):
        out = out + taps[k : k + 1] * buf[pl.ds(5 + k, Q), :]
    return out


def softplus(v):
    return jnp.maximum(v, 0.0) + jnp.log1p(jnp.exp(-jnp.abs(v)))


def spread(columns, pair, low_half):
    first = jnp.broadcast_to(columns[:, 2 * pair : 2 * pair + 1], (columns.shape[0], 2 * WIDTH))
    second = jnp.broadcast_to(
        columns[:, 2 * pair + 1 : 2 * pair + 2], (columns.shape[0], 2 * WIDTH)
    )
    return first, second, jnp.where(low_half[: columns.shape[0]], first, second)


def forward_kernel(
    inner_ref, small_ref, xw_ref, xb_ref, bcw_ref, bcb_ref, bias_ref, alog_ref, skip_ref,
    pack_ref, rows_ref,
    y_ref, state_out_ref, all_ref, tokens_ref,
    xbuf, bcbuf, state, mixed, weighted, ls, lr, ll, qs, qr, ql,
):
    step = pl.program_id(0)
    heads = bias_ref.shape[1]
    line = LineGather(pack_ref, all_ref, ls, lr, ll)
    quad = QuadGather(rows_ref, tokens_ref, qs, qr, ql)

    @pl.when(step == 0)
    def _():
        greet(True, True)
        line.start()
        quad.start()

    @pl.when(step == 0)
    def _():
        state[...] = jnp.zeros_like(state)
        xbuf[0:8, :] = jnp.zeros((8, xbuf.shape[1]), F32)
        bcbuf[0:8, :] = jnp.zeros((8, bcbuf.shape[1]), F32)

    xbuf[8:, :] = inner_ref[...]
    bcbuf[8:, :] = small_ref[:, : 2 * STATE]
    row, col = tri_masks()
    causal = row >= col
    low_half = col < WIDTH
    pre_bc = conv_block(bcbuf, bcw_ref[...], bcb_ref[...])
    bc = low(pre_bc * jax.nn.sigmoid(pre_bc))
    b, c = bc[:, :STATE], bc[:, STATE:]
    dt = softplus(small_ref[:, 2 * STATE :] + bias_ref[...])
    decay = dt * -jnp.exp(alog_ref[...])
    cum = dot(causal.astype(F32), decay, precision=HIGHEST)
    cum_t = cum.T
    scores = dot(c, b, ((1,), (1,)))
    state_low = low(state[...])
    state_out_ref[0] = state[...]
    carried = dot(c, state_low)
    xw, xb = xw_ref[...], xb_ref[...]
    skip = skip_ref[...]
    for pair in range(heads // 2):
        sl = slice(2 * WIDTH * pair, 2 * WIDTH * (pair + 1))
        pre = xb[:, sl] + xw[0:1, sl] * xbuf[pl.ds(5, Q), sl]
        for k in range(1, 4):
            pre = pre + xw[k : k + 1, sl] * xbuf[pl.ds(5 + k, Q), sl]
        x = pre * jax.nn.sigmoid(pre)
        _, _, dt_e = spread(dt, pair, low_half)
        _, _, skip_e = spread(skip, pair, low_half)
        cum_0, cum_1, cum_e = spread(cum, pair, low_half)
        xh = x * dt_e
        parts = []
        for h, cum_h in ((2 * pair, cum_0), (2 * pair + 1, cum_1)):
            gap = cum_h - cum_t[h : h + 1, :]
            parts.append(low(jnp.exp(jnp.where(causal, gap, NEG)) * scores))
        xl = low(xh)
        zero = jnp.zeros_like(xl)
        stacked = jnp.concatenate([jnp.where(low_half, xl, zero), jnp.where(low_half, zero, xl)], 0)
        y = dot(jnp.concatenate(parts, 1), stacked)
        last = cum_e[Q - 1 : Q, :]
        y = y + carried[:, sl] * jnp.exp(cum_e) + skip_e * x
        y_ref[:, sl] = y
        weighted[:, sl] = low(xh * jnp.exp(last - cum_e))
        mixed[:, sl] = jnp.exp(last)
    state[...] = state[...] * mixed[...] + dot(b.T, weighted[...])
    xbuf[0:8, :] = xbuf[Q : Q + 8, :]
    bcbuf[0:8, :] = bcbuf[Q : Q + 8, :]

    @pl.when(step == pl.num_programs(0) - 1)
    def _():
        for hop in range(1, line.nz):
            line.relay(hop)
            if hop == 1:
                quad.relay()
        quad.finish()
        line.finish()


def full(shape):
    return pl.BlockSpec(shape, lambda i: (0,) * len(shape))


def mixer_forward(inner, small, xw, xb, bcw, bcb, bias, alog, skip, pack, tokens):
    n = lax.axis_size("dp")
    far = pl.BlockSpec(memory_space=pl.ANY)
    rows, channels = inner.shape
    blocks = rows // Q
    wide = small.shape[1]
    return pl.pallas_call(
        forward_kernel,
        name="mixer_forward",
        grid=(blocks,),
        in_specs=[
            pl.BlockSpec((Q, channels), lambda i: (i, 0)),
            pl.BlockSpec((Q, wide), lambda i: (i, 0)),
            full(xw.shape), full(xb.shape), full(bcw.shape), full(bcb.shape),
            full(bias.shape), full(alog.shape), full(skip.shape),
            full(pack.shape), full(tokens.shape),
        ],
        out_specs=[
            pl.BlockSpec((Q, channels), lambda i: (i, 0)),
            pl.BlockSpec((1, STATE, channels), lambda i: (i, 0, 0)),
            far,
            far,
        ],
        out_shape=[
            jax.ShapeDtypeStruct((rows, channels), F32),
            jax.ShapeDtypeStruct((blocks, STATE, channels), F32),
            jax.ShapeDtypeStruct((n,) + pack.shape, pack.dtype),
            jax.ShapeDtypeStruct((4,) + tokens.shape, tokens.dtype),
        ],
        scratch_shapes=[
            pltpu.VMEM((Q + 8, channels), F32),
            pltpu.VMEM((Q + 8, 2 * STATE), F32),
            pltpu.VMEM((STATE, channels), F32),
            pltpu.VMEM((1, channels), F32),
            pltpu.VMEM((Q, channels), BF16),
        ]
        + line_semaphores(n)
        + quad_semaphores(),
        compiler_params=pltpu.CompilerParams(collective_id=1, has_side_effects=True),
        cost_estimate=pl.CostEstimate(
            flops=rows * channels * Q * 8, bytes_accessed=rows * channels * 16, transcendentals=rows * channels * 8
        ),
    )(inner, small, xw, xb, bcw, bcb, bias, alog, skip, pack, tokens)


def backward_kernel(
    inner_ref, prev_ref, small_ref, sprev_ref, gy_ref, state_ref,
    xw_ref, xb_ref, bcw_ref, bcb_ref, bias_ref, alog_ref, skip_ref,
    dinner_ref, ddt_ref, dbc_ref, gxw_ref, gbcw_ref, ghead_ref,
    xbuf, bcbuf, dxbuf, dbcbuf, dstate, carried, back, rows_buf, sums, cgy, weighted, decay_row,
):
    step = pl.program_id(0)
    blocks = pl.num_programs(0)
    heads = bias_ref.shape[1]
    channels = inner_ref.shape[1]

    @pl.when(step == 0)
    def _():
        dstate[...] = jnp.zeros_like(dstate)
        dxbuf[Q:, :] = jnp.zeros((8, channels), F32)
        dbcbuf[Q:, :] = jnp.zeros((8, 2 * STATE), F32)
        gxw_ref[...] = jnp.zeros_like(gxw_ref)
        gbcw_ref[...] = jnp.zeros_like(gbcw_ref)
        ghead_ref[...] = jnp.zeros_like(ghead_ref)

    first = step == blocks - 1
    xbuf[0:8, :] = jnp.where(first, 0.0, prev_ref[...])
    bcbuf[0:8, :] = jnp.where(first, 0.0, sprev_ref[:, : 2 * STATE])
    xbuf[8:, :] = inner_ref[...]
    bcbuf[8:, :] = small_ref[:, : 2 * STATE]
    row, col = tri_masks()
    causal = row >= col
    causal_t = col >= row
    low_half = col < WIDTH
    pre_bc = conv_block(bcbuf, bcw_ref[...], bcb_ref[...])
    sig_bc = jax.nn.sigmoid(pre_bc)
    bc = low(pre_bc * sig_bc)
    b, c = bc[:, :STATE], bc[:, STATE:]
    raw = small_ref[:, 2 * STATE :] + bias_ref[...]
    dt = softplus(raw)
    a = -jnp.exp(alog_ref[...])
    cum = dot(causal.astype(F32), dt * a, precision=HIGHEST)
    cum_t = cum.T
    scores_t = dot(b, c, ((1,), (1,)))
    dstate_low = low(dstate[...])
    state_low = low(state_ref[0])
    carried[...] = dot(c, state_low)
    back[...] = dot(b, dstate_low)
    xw, xb = xw_ref[...], xb_ref[...]
    skip = skip_ref[...]
    dscores_t = jnp.zeros((Q, Q), F32)
    cols = jnp.zeros((Q, heads), F32)
    hot_row = lax.broadcasted_iota(jnp.int32, (2 * Q, heads), 0) // Q
    hot_col = lax.broadcasted_iota(jnp.int32, (2 * Q, heads), 1)
    for pair in range(heads // 2):
        sl = slice(2 * WIDTH * pair, 2 * WIDTH * (pair + 1))
        shifted = [xbuf[pl.ds(5 + k, Q), sl] for k in range(4)]
        pre = xb[:, sl] + xw[0:1, sl] * shifted[0]
        for k in range(1, 4):
            pre = pre + xw[k : k + 1, sl] * shifted[k]
        sig = jax.nn.sigmoid(pre)
        x = pre * sig
        _, _, dt_e = spread(dt, pair, low_half)
        _, _, skip_e = spread(skip, pair, low_half)
        cum_0, cum_1, cum_e = spread(cum, pair, low_half)
        last = cum_e[Q - 1 : Q, :]
        xh = x * dt_e
        xl = low(xh)
        gy = gy_ref[:, sl]
        gl = low(gy)
        zero = jnp.zeros_like(gl)
        g_stack = jnp.concatenate([jnp.where(low_half, gl, zero), jnp.where(low_half, zero, gl)], 0)
        dmixed_t = dot(xl, g_stack, ((1,), (1,)))
        mixes, zs = [], []
        for i, (h, cum_h) in enumerate(((2 * pair, cum_0), (2 * pair + 1, cum_1))):
            gap = cum_t[h : h + 1, :] - cum_h
            within = jnp.exp(jnp.where(causal_t, gap, NEG))
            mix = within * scores_t
            dm = dmixed_t[:, i * Q : (i + 1) * Q]
            dscores_t = dscores_t + dm * within
            z = low(dm * mix)
            zs.append(z)
            mixes.append(low(mix))
            rows_buf[h : h + 1, :] = jnp.sum(z.astype(F32), axis=0, keepdims=True)
        hot = (hot_col == hot_row + 2 * pair).astype(BF16)
        cols = cols + dot(jnp.concatenate(zs, 1), hot)
        dxh = dot(jnp.concatenate(mixes, 1), g_stack)
        to_end = jnp.exp(last - cum_e)
        from_state = to_end * back[:, sl]
        dxh = dxh + from_state
        grown = jnp.exp(cum_e) * gy
        cgy[:, sl] = low(grown)
        weighted[:, sl] = low(xh * to_end)
        sums[0:Q, sl] = low(grown * carried[:, sl])
        sums[Q : 2 * Q, sl] = low(xh * from_state)
        sums[2 * Q : 3 * Q, sl] = low(dxh * x)
        sums[3 * Q : 4 * Q, sl] = low(gy * x)
        decay_row[:, sl] = jnp.exp(last)
        dx = dxh * dt_e + skip_e * gy
        dpre = dx * (sig * (1.0 + pre * (1.0 - sig)))
        dxbuf[0:Q, sl] = dpre
        out = xw[3:4, sl] * dpre
        for k in range(3):
            out = out + xw[k : k + 1, sl] * dxbuf[pl.ds(3 - k, Q), sl]
        dinner_ref[:, sl] = low(out)
        for k in range(4):
            gxw_ref[k : k + 1, sl] += jnp.sum(dpre * shifted[k], axis=0, keepdims=True)
        gxw_ref[4:5, sl] += jnp.sum(dpre, axis=0, keepdims=True)
    head_of = lax.broadcasted_iota(jnp.int32, (channels, heads), 0) // WIDTH
    head = lax.broadcasted_iota(jnp.int32, (channels, heads), 1)
    head_hot = (head_of == head).astype(BF16)
    head_sums = dot(sums[...], head_hot)
    v, u = head_sums[0:Q], head_sums[Q : 2 * Q]
    t_x, t_skip = head_sums[2 * Q : 3 * Q], head_sums[3 * Q :]
    kept = jnp.sum(dstate[...] * state_ref[0], axis=0, keepdims=True) * decay_row[...]
    dlast = dot(jnp.broadcast_to(kept, (8, channels)), head_hot.astype(F32), precision=HIGHEST)[0:1]
    dlast = dlast + jnp.sum(u, axis=0, keepdims=True)
    dcum = rows_buf[0:heads, :].T - cols + v - u
    ddecay = dot(causal_t.astype(F32), dcum, precision=HIGHEST) + dlast
    ddt = (ddecay * a + t_x) * jax.nn.sigmoid(raw)
    ddt_ref[...] = low(ddt)
    ghead_ref[0:1, :] += jnp.sum(ddt, axis=0, keepdims=True)
    ghead_ref[1:2, :] += jnp.sum(ddecay * dt, axis=0, keepdims=True) * a
    ghead_ref[2:3, :] += jnp.sum(t_skip, axis=0, keepdims=True)
    dsl = low(dscores_t)
    dc = dot(dsl, b, ((0,), (0,))) + dot(cgy[...], state_low, ((1,), (1,)))
    db = dot(dsl, c) + dot(weighted[...], dstate_low, ((1,), (1,)))
    dstate[...] = dstate[...] * decay_row[...] + dot(c.T, cgy[...])
    dbc = jnp.concatenate([db, dc], 1)
    dpre = dbc * (sig_bc * (1.0 + pre_bc * (1.0 - sig_bc)))
    dbcbuf[0:Q, :] = dpre
    bcw = bcw_ref[...]
    out = bcw[3:4] * dpre
    for k in range(3):
        out = out + bcw[k : k + 1] * dbcbuf[pl.ds(3 - k, Q), :]
    dbc_ref[...] = out.astype(dbc_ref.dtype)
    for k in range(4):
        gbcw_ref[k : k + 1, :] += jnp.sum(dpre * bcbuf[pl.ds(5 + k, Q), :], axis=0, keepdims=True)
    gbcw_ref[4:5, :] += jnp.sum(dpre, axis=0, keepdims=True)
    dxbuf[Q:, :] = dxbuf[0:8, :]
    dbcbuf[Q:, :] = dbcbuf[0:8, :]


def mixer_backward(inner, small, gy, states, xw, xb, bcw, bcb, bias, alog, skip, dbc_dtype=F32):
    rows, channels = inner.shape
    blocks = rows // Q
    wide = small.shape[1]
    heads = bias.shape[1]
    at = lambda i: blocks - 1 - i
    before = lambda i: jnp.maximum(at(i) * (Q // 8) - 1, 0)
    return pl.pallas_call(
        backward_kernel,
        name="mixer_backward",
        grid=(blocks,),
        in_specs=[
            pl.BlockSpec((Q, channels), lambda i: (at(i), 0)),
            pl.BlockSpec((8, channels), lambda i: (before(i), 0)),
            pl.BlockSpec((Q, wide), lambda i: (at(i), 0)),
            pl.BlockSpec((8, wide), lambda i: (before(i), 0)),
            pl.BlockSpec((Q, channels), lambda i: (at(i), 0)),
            pl.BlockSpec((1, STATE, channels), lambda i: (at(i), 0, 0)),
            full(xw.shape), full(xb.shape), full(bcw.shape), full(bcb.shape),
            full(bias.shape), full(alog.shape), full(skip.shape),
        ],
        out_specs=[
            pl.BlockSpec((Q, channels), lambda i: (at(i), 0)),
            pl.BlockSpec((Q, heads), lambda i: (at(i), 0)),
            pl.BlockSpec((Q, 2 * STATE), lambda i: (at(i), 0)),
            full((5, channels)), full((5, 2 * STATE)), full((3, heads)),
        ],
        out_shape=[
            jax.ShapeDtypeStruct((rows, channels), BF16),
            jax.ShapeDtypeStruct((rows, heads), BF16),
            jax.ShapeDtypeStruct((rows, 2 * STATE), dbc_dtype),
            jax.ShapeDtypeStruct((5, channels), F32),
            jax.ShapeDtypeStruct((5, 2 * STATE), F32),
            jax.ShapeDtypeStruct((3, heads), F32),
        ],
        scratch_shapes=[
            pltpu.VMEM((Q + 8, channels), F32),
            pltpu.VMEM((Q + 8, 2 * STATE), F32),
            pltpu.VMEM((Q + 8, channels), F32),
            pltpu.VMEM((Q + 8, 2 * STATE), F32),
            pltpu.VMEM((STATE, channels), F32),
            pltpu.VMEM((Q, channels), F32),
            pltpu.VMEM((Q, channels), F32),
            pltpu.VMEM((16, Q), F32),
            pltpu.VMEM((4 * Q, channels), BF16),
            pltpu.VMEM((Q, channels), BF16),
            pltpu.VMEM((Q, channels), BF16),
            pltpu.VMEM((1, channels), F32),
        ],
        cost_estimate=pl.CostEstimate(
            flops=rows * channels * Q * 20, bytes_accessed=rows * channels * 20, transcendentals=rows * channels * 10
        ),
    )(inner, inner, small, small, gy, states, xw, xb, bcw, bcb, bias, alog, skip)


def remote(src, dst, send, recv, **to):
    return pltpu.make_async_remote_copy(
        src_ref=src, dst_ref=dst, send_sem=send, recv_sem=recv, device_id=to, device_id_type=MESH
    )


def line_place():
    me = lax.axis_index("dp")
    return me // 2, me % 2, lax.axis_size("dp") // 2


def quad_place():
    me = lax.axis_index("tensor")
    x, core = me // 2, me % 2
    return me, x * 2 + 1 - core, (1 - x) * 2 + core, (1 - x) * 2 + 1 - core


def greet(line, quad):
    barrier = pltpu.get_barrier_semaphore()
    count = 0
    if line:
        z, y, nz = line_place()
        pl.semaphore_signal(barrier, inc=1, device_id={"dp": z * 2 + 1 - y}, device_id_type=MESH)
        count = 1

        @pl.when(z > 0)
        def _():
            pl.semaphore_signal(barrier, inc=1, device_id={"dp": z * 2 - 2 + y}, device_id_type=MESH)

        @pl.when(z < nz - 1)
        def _():
            pl.semaphore_signal(barrier, inc=1, device_id={"dp": z * 2 + 2 + y}, device_id_type=MESH)

        count = count + jnp.where(z > 0, 1, 0) + jnp.where(z < nz - 1, 1, 0)
    if quad:
        _, partner, across, _ = quad_place()
        pl.semaphore_signal(barrier, inc=1, device_id={"tensor": partner}, device_id_type=MESH)
        pl.semaphore_signal(barrier, inc=1, device_id={"tensor": across}, device_id_type=MESH)
        count = count + 2
    pl.semaphore_wait(barrier, count)


class LineGather:
    def __init__(self, own, out, send, recv, local):
        self.own, self.out, self.send, self.recv = own, out, send, recv
        self.z, self.y, self.nz = line_place()
        self.local = pltpu.make_async_copy(own, out.at[self.z * 2 + self.y], local)

    def copy(self, z, y, way, src=None):
        slot = z * 2 + y
        to = (self.z * 2 + 2 + self.y, self.z * 2 - 2 + self.y, self.z * 2 + 1 - self.y)[way]
        return remote(
            self.out.at[slot] if src is None else src,
            self.out.at[slot],
            self.send.at[slot, way],
            self.recv.at[slot],
            dp=to,
        )

    def each(self, act):
        z, y, nz = self.z, self.y, self.nz
        pl.when(z < nz - 1)(lambda: act(self.copy(z, y, 0, self.own)))
        pl.when(z > 0)(lambda: act(self.copy(z, y, 1, self.own)))
        act(self.copy(z, y, 2, self.own))

    def start(self):
        self.each(lambda c: c.start())
        self.local.start()

    def relay(self, hop):
        z, y, nz = self.z, self.y, self.nz

        @pl.when(z >= hop)
        def _():
            self.copy(z - hop, y, 2).wait_recv()
            pl.when(z < nz - 1)(lambda: self.copy(z - hop, y, 0).start())
            self.copy(z - hop, y, 2).start()

        @pl.when(z + hop < nz)
        def _():
            self.copy(z + hop, y, 2).wait_recv()
            pl.when(z > 0)(lambda: self.copy(z + hop, y, 1).start())
            self.copy(z + hop, y, 2).start()

    def finish(self):
        z, y, nz = self.z, self.y, self.nz
        for other in range(nz):
            self.copy(other, 1 - y, 2).wait_recv()
        self.local.wait()
        self.each(lambda c: c.wait_send())
        for hop in range(1, nz):

            @pl.when(z >= hop)
            def _():
                pl.when(z < nz - 1)(lambda: self.copy(z - hop, y, 0).wait_send())
                self.copy(z - hop, y, 2).wait_send()

            @pl.when(z + hop < nz)
            def _():
                pl.when(z > 0)(lambda: self.copy(z + hop, y, 1).wait_send())
                self.copy(z + hop, y, 2).wait_send()


class QuadGather:
    def __init__(self, own, out, send, recv, local):
        self.own, self.out, self.send, self.recv = own, out, send, recv
        self.me, self.partner, self.over, self.diagonal = quad_place()
        self.local = pltpu.make_async_copy(own, out.at[self.me], local)

    def copy(self, slot, src, way, to):
        return remote(src, self.out.at[slot], self.send.at[way], self.recv.at[slot], tensor=to)

    def sends(self):
        return (
            self.copy(self.me, self.own, 0, self.over),
            self.copy(self.me, self.own, 1, self.partner),
            self.copy(self.over, self.out.at[self.over], 2, self.partner),
        )

    def arrival(self, slot):
        return self.copy(slot, self.own, 0, self.partner)

    def start(self):
        across, beside, _ = self.sends()
        across.start()
        beside.start()
        self.local.start()

    def relay(self):
        self.arrival(self.over).wait_recv()
        self.sends()[2].start()

    def finish(self):
        self.arrival(self.partner).wait_recv()
        self.arrival(self.diagonal).wait_recv()
        self.local.wait()
        for send in self.sends():
            send.wait_send()


def line_semaphores(n):
    return [
        pltpu.SemaphoreType.DMA((n, 3)),
        pltpu.SemaphoreType.DMA((n,)),
        pltpu.SemaphoreType.DMA,
    ]


def quad_semaphores():
    return [
        pltpu.SemaphoreType.DMA((3,)),
        pltpu.SemaphoreType.DMA((4,)),
        pltpu.SemaphoreType.DMA,
    ]


def first_kernel(pack_ref, rows_ref, all_ref, tokens_ref, ls, lr, ll, qs, qr, ql):
    greet(True, True)
    line = LineGather(pack_ref, all_ref, ls, lr, ll)
    quad = QuadGather(rows_ref, tokens_ref, qs, qr, ql)
    line.start()
    quad.start()
    for hop in range(1, line.nz):
        line.relay(hop)
        if hop == 1:
            quad.relay()
    quad.finish()
    line.finish()


def gather_first(pack, rows):
    n = lax.axis_size("dp")
    whole = pl.BlockSpec(memory_space=pltpu.VMEM)
    far = pl.BlockSpec(memory_space=pl.ANY)
    return pl.pallas_call(
        first_kernel,
        name="gather_first",
        in_specs=[whole, whole],
        out_specs=[far, far],
        out_shape=[
            jax.ShapeDtypeStruct((n,) + pack.shape, pack.dtype),
            jax.ShapeDtypeStruct((4,) + rows.shape, rows.dtype),
        ],
        scratch_shapes=line_semaphores(n) + quad_semaphores(),
        compiler_params=pltpu.CompilerParams(collective_id=0, has_side_effects=True),
    )(pack, rows)


def local(
    hidden_in, d_out, in_gain, w_zx, w_dt, w_bc, w_out,
    conv_x_w, conv_x_b, conv_bc_w, conv_bc_b, dt_bias, a_log, d_skip, norm_scale,
):
    _, rows_local, width = hidden_in.shape
    inner_local = w_zx.shape[2]
    heads = w_dt.shape[1]
    tensor_index = lax.axis_index("tensor")
    parts = lax.axis_size("tensor")
    own_width = in_gain.shape[0]
    spare = jnp.zeros((own_width, 127 - heads), BF16)
    first_pack = jnp.concatenate([w_zx[:, 1, :], w_bc, w_dt, in_gain[:, None], spare], 1)
    first, hidden_bf = gather_first(first_pack, hidden_in[0])
    first = first.reshape(width, -1)
    hidden_bf = hidden_bf.reshape(-1, width)
    second_pack = jnp.concatenate([w_zx[:, 0, :], w_out], 1)
    w_inner = first[:, :inner_local]
    w_small = first[:, inner_local : inner_local + 2 * STATE + heads]
    gain = first[:, inner_local + 2 * STATE + heads].astype(F32)[None]

    hidden = hidden_bf.astype(F32)
    rh = lax.rsqrt(jnp.mean(hidden * hidden, axis=-1, keepdims=True) + EPSILON)
    xn = low(hidden * rh * gain)
    inner = dot(xn, w_inner)
    small = dot(xn, w_small)
    params = (
        conv_x_w, conv_x_b[None], conv_bc_w, conv_bc_b[None], dt_bias[None], a_log[None], d_skip[None],
    )
    y, states, second, dout_all = mixer_forward(inner, small, *params, second_pack, d_out[0])
    second = second.reshape(width, -1)
    dout_all = dout_all.reshape(-1, width)
    w_gate, w_o = second[:, :inner_local], second[:, inner_local:]
    gate = dot(xn, w_gate)
    dyn = dot(dout_all, w_o)
    sig = jax.nn.sigmoid(gate)
    act = gate * sig
    gated = y * act
    scale = norm_scale[None]
    scaled = dyn * scale
    sums = lax.psum(jnp.stack([jnp.sum(gated * gated, -1), jnp.sum(scaled * gated, -1)]), "tensor")
    channels = inner_local * parts
    r = lax.rsqrt(sums[0] / channels + EPSILON)[:, None]
    yn = low(gated * r * scale)
    d_gated = r * scaled - gated * (r * r * r) * sums[1][:, None] / channels
    g_scale = jnp.sum(dyn * gated * r, axis=0)
    gy = d_gated * act
    d_gate = low(d_gated * y * (sig * (1.0 + gate * (1.0 - sig))))
    g_out = low(dot(dout_all, yn, ((0,), (0,))))
    g_gate = low(dot(xn, d_gate, ((0,), (0,))))
    early = lax.psum_scatter(
        jnp.concatenate([g_gate, g_out], 1), "dp", scatter_dimension=0, tiled=True
    ).astype(F32)
    partial_out = low(dot(yn, w_o, ((1,), (1,))))
    branch = lax.psum_scatter(partial_out, "tensor", scatter_dimension=0, tiled=True)
    hidden_own = hidden_in[0].astype(F32)
    block_out = low(hidden_own + branch.astype(F32))

    d_inner, d_dt, d_bc, g_x, g_bc, g_head = mixer_backward(
        inner, small, gy, states, *params, dbc_dtype=BF16
    )
    d_bc_low = lax.psum(d_bc, "tensor")
    own_columns = 2 * STATE // parts
    d_bc_own = lax.dynamic_slice_in_dim(d_bc_low, tensor_index * own_columns, own_columns, 1)
    late = jnp.concatenate([d_inner, d_bc_own, d_dt], 1)
    g_late = low(dot(xn, late, ((0,), (0,))))
    late_sum = lax.psum_scatter(g_late, "dp", scatter_dimension=0, tiled=True).astype(F32)
    w_small_own = jnp.concatenate(
        [
            lax.dynamic_slice_in_dim(first, inner_local + tensor_index * own_columns, own_columns, 1),
            w_small[:, 2 * STATE :],
        ],
        1,
    )
    d_xn = dot(d_gate, w_gate, ((1,), (1,))) + dot(d_inner, w_inner, ((1,), (1,)))
    d_xn = d_xn + dot(late[:, inner_local:], w_small_own, ((1,), (1,)))
    d_normed = lax.psum_scatter(low(d_xn), "tensor", scatter_dimension=0, tiled=True).astype(F32)
    rh_own = lax.rsqrt(jnp.mean(hidden_own * hidden_own, axis=-1, keepdims=True) + EPSILON)
    weighted = d_normed * gain
    g_gain = jnp.sum(d_normed * hidden_own * rh_own, axis=0)
    inner_sum = jnp.sum(weighted * hidden_own, axis=-1, keepdims=True)
    d_hidden = (
        d_out[0].astype(F32) + rh_own * weighted - hidden_own * (rh_own * rh_own * rh_own) * inner_sum / width
    )
    flat = jnp.concatenate(
        [g_gain, g_bc.reshape(-1), g_x.reshape(-1), g_scale, g_head.reshape(-1)]
    )
    flat = lax.psum(flat, "dp")
    shared_size = width + 5 * 2 * STATE
    shared = lax.psum(flat[:shared_size], "tensor")
    own = lax.dynamic_slice_in_dim(shared, lax.axis_index("dp") * in_gain.shape[0], in_gain.shape[0], 0)
    g_bc = shared[width:].reshape(5, 2 * STATE)
    g_x = flat[shared_size : shared_size + 5 * inner_local].reshape(5, inner_local)
    rest = flat[shared_size + 5 * inner_local :]
    g_scale = rest[:inner_local]
    g_head = rest[inner_local:].reshape(3, heads)
    g_w_bc = lax.all_gather(late_sum[:, inner_local : inner_local + own_columns], "tensor", axis=1, tiled=True)
    g_zx = jnp.stack([early[:, :inner_local], late_sum[:, :inner_local]], 1)
    return (
        block_out[None],
        d_hidden[None],
        own,
        g_zx,
        late_sum[:, inner_local + own_columns :],
        g_w_bc,
        early[:, inner_local:],
        g_x[:4],
        g_x[4],
        g_bc[:4],
        g_bc[4],
        g_head[0],
        g_head[1],
        g_head[2],
        g_scale,
    )


def solution(mesh):
    tokens = P("dp", "tensor", None)
    specs = (
        tokens,
        tokens,
        P("dp"),
        P("dp", None, "tensor"),
        P("dp", "tensor"),
        P("dp", None),
        P("dp", "tensor"),
        P(None, "tensor"),
        P("tensor"),
        P(),
        P(),
        P("tensor"),
        P("tensor"),
        P("tensor"),
        P("tensor"),
    )
    return jax.shard_map(local, mesh=mesh, in_specs=specs, out_specs=specs, check_vma=False)
```

```python
import jax
import jax.numpy as jnp
from jax import lax
from jax.experimental import pallas as pl
from jax.experimental.pallas import tpu as pltpu
from jax.sharding import PartitionSpec as P

Q = 128
STATE = 128
WIDTH = 64
NEG = -1e30
EPSILON = 1e-05
MESH = pl.DeviceIdType.MESH
HIGHEST = lax.Precision.HIGHEST
F32 = jnp.float32
BF16 = jnp.bfloat16


def dot(a, b, dims=((1,), (0,)), precision=None):
    return lax.dot_general(a, b, (dims, ((), ())), precision=precision, preferred_element_type=F32)


def low(v):
    return v.astype(BF16)


def tri_masks():
    row = lax.broadcasted_iota(jnp.int32, (Q, Q), 0)
    col = lax.broadcasted_iota(jnp.int32, (Q, Q), 1)
    return row, col


def conv_block(buf, taps, bias):
    out = bias + taps[0:1] * buf[pl.ds(5, Q), :]
    for k in range(1, 4):
        out = out + taps[k : k + 1] * buf[pl.ds(5 + k, Q), :]
    return out


def softplus(v):
    return jnp.maximum(v, 0.0) + jnp.log1p(jnp.exp(-jnp.abs(v)))


def spread(columns, pair, low_half):
    first = jnp.broadcast_to(columns[:, 2 * pair : 2 * pair + 1], (columns.shape[0], 2 * WIDTH))
    second = jnp.broadcast_to(
        columns[:, 2 * pair + 1 : 2 * pair + 2], (columns.shape[0], 2 * WIDTH)
    )
    return first, second, jnp.where(low_half[: columns.shape[0]], first, second)


def forward_kernel(
    inner_ref, small_ref, xw_ref, xb_ref, bcw_ref, bcb_ref, bias_ref, alog_ref, skip_ref,
    pack_ref, rows_ref,
    y_ref, state_out_ref, all_ref, tokens_ref,
    xbuf, bcbuf, state, mixed, weighted, ls, lr, ll, qs, qr, ql,
):
    step = pl.program_id(0)
    heads = bias_ref.shape[1]
    line = LineGather(pack_ref, all_ref, ls, lr, ll)
    quad = QuadGather(rows_ref, tokens_ref, qs, qr, ql)

    @pl.when(step == 0)
    def _():
        greet(True, True)
        line.start()
        quad.start()

    @pl.when(step == 0)
    def _():
        state[...] = jnp.zeros_like(state)
        xbuf[0:8, :] = jnp.zeros((8, xbuf.shape[1]), F32)
        bcbuf[0:8, :] = jnp.zeros((8, bcbuf.shape[1]), F32)

    xbuf[8:, :] = inner_ref[...]
    bcbuf[8:, :] = small_ref[:, : 2 * STATE]
    row, col = tri_masks()
    causal = row >= col
    low_half = col < WIDTH
    pre_bc = conv_block(bcbuf, bcw_ref[...], bcb_ref[...])
    bc = low(pre_bc * jax.nn.sigmoid(pre_bc))
    b, c = bc[:, :STATE], bc[:, STATE:]
    dt = softplus(small_ref[:, 2 * STATE :] + bias_ref[...])
    decay = dt * -jnp.exp(alog_ref[...])
    cum = dot(causal.astype(F32), decay, precision=HIGHEST)
    cum_t = cum.T
    scores = dot(c, b, ((1,), (1,)))
    state_low = low(state[...])
    state_out_ref[0] = state[...]
    carried = dot(c, state_low)
    xw, xb = xw_ref[...], xb_ref[...]
    skip = skip_ref[...]
    for pair in range(heads // 2):
        sl = slice(2 * WIDTH * pair, 2 * WIDTH * (pair + 1))
        pre = xb[:, sl] + xw[0:1, sl] * xbuf[pl.ds(5, Q), sl]
        for k in range(1, 4):
            pre = pre + xw[k : k + 1, sl] * xbuf[pl.ds(5 + k, Q), sl]
        x = pre * jax.nn.sigmoid(pre)
        _, _, dt_e = spread(dt, pair, low_half)
        _, _, skip_e = spread(skip, pair, low_half)
        cum_0, cum_1, cum_e = spread(cum, pair, low_half)
        xh = x * dt_e
        parts = []
        for h, cum_h in ((2 * pair, cum_0), (2 * pair + 1, cum_1)):
            gap = cum_h - cum_t[h : h + 1, :]
            parts.append(low(jnp.exp(jnp.where(causal, gap, NEG)) * scores))
        xl = low(xh)
        zero = jnp.zeros_like(xl)
        stacked = jnp.concatenate([jnp.where(low_half, xl, zero), jnp.where(low_half, zero, xl)], 0)
        y = dot(jnp.concatenate(parts, 1), stacked)
        last = cum_e[Q - 1 : Q, :]
        y = y + carried[:, sl] * jnp.exp(cum_e) + skip_e * x
        y_ref[:, sl] = y
        weighted[:, sl] = low(xh * jnp.exp(last - cum_e))
        mixed[:, sl] = jnp.exp(last)
    state[...] = state[...] * mixed[...] + dot(b.T, weighted[...])
    xbuf[0:8, :] = xbuf[Q : Q + 8, :]
    bcbuf[0:8, :] = bcbuf[Q : Q + 8, :]

    @pl.when(step == pl.num_programs(0) - 1)
    def _():
        for hop in range(1, line.nz):
            line.relay(hop)
            if hop == 1:
                quad.relay()
        quad.finish()
        line.finish()


def full(shape):
    return pl.BlockSpec(shape, lambda i: (0,) * len(shape))


def mixer_forward(inner, small, xw, xb, bcw, bcb, bias, alog, skip, pack, tokens):
    n = lax.axis_size("dp")
    far = pl.BlockSpec(memory_space=pl.ANY)
    rows, channels = inner.shape
    blocks = rows // Q
    wide = small.shape[1]
    return pl.pallas_call(
        forward_kernel,
        name="mixer_forward",
        grid=(blocks,),
        in_specs=[
            pl.BlockSpec((Q, channels), lambda i: (i, 0)),
            pl.BlockSpec((Q, wide), lambda i: (i, 0)),
            full(xw.shape), full(xb.shape), full(bcw.shape), full(bcb.shape),
            full(bias.shape), full(alog.shape), full(skip.shape),
            full(pack.shape), full(tokens.shape),
        ],
        out_specs=[
            pl.BlockSpec((Q, channels), lambda i: (i, 0)),
            pl.BlockSpec((1, STATE, channels), lambda i: (i, 0, 0)),
            far,
            far,
        ],
        out_shape=[
            jax.ShapeDtypeStruct((rows, channels), F32),
            jax.ShapeDtypeStruct((blocks, STATE, channels), F32),
            jax.ShapeDtypeStruct((n,) + pack.shape, pack.dtype),
            jax.ShapeDtypeStruct((4,) + tokens.shape, tokens.dtype),
        ],
        scratch_shapes=[
            pltpu.VMEM((Q + 8, channels), F32),
            pltpu.VMEM((Q + 8, 2 * STATE), F32),
            pltpu.VMEM((STATE, channels), F32),
            pltpu.VMEM((1, channels), F32),
            pltpu.VMEM((Q, channels), BF16),
        ]
        + line_semaphores(n)
        + quad_semaphores(),
        compiler_params=pltpu.CompilerParams(collective_id=1, has_side_effects=True),
        cost_estimate=pl.CostEstimate(
            flops=rows * channels * Q * 8, bytes_accessed=rows * channels * 16, transcendentals=rows * channels * 8
        ),
    )(inner, small, xw, xb, bcw, bcb, bias, alog, skip, pack, tokens)


def backward_kernel(
    inner_ref, prev_ref, small_ref, sprev_ref, gy_ref, state_ref,
    xw_ref, xb_ref, bcw_ref, bcb_ref, bias_ref, alog_ref, skip_ref,
    gate_grad_ref, out_grad_ref, branch_part_ref,
    dinner_ref, ddt_ref, dbc_ref, grads_ref, gate_sum_ref, out_sum_ref, branch_ref,
    xbuf, bcbuf, dxbuf, dbcbuf, dstate, carried, back, rows_buf, sums, cgy, weighted, decay_row,
    dbc_mine, dbc_there, bsend, brecv, *scratch,
):
    step = pl.program_id(0)
    blocks = pl.num_programs(0)
    me, partner, over, diagonal = quad_place()
    gate_scatter = LineScatter(gate_grad_ref, gate_sum_ref, *scratch[0:5])
    out_scatter = LineScatter(out_grad_ref, out_sum_ref, *scratch[5:10])
    branch = QuadScatter(branch_part_ref, branch_ref, *scratch[10:14])
    hops = list(range(out_scatter.nz - 1, 0, -1))
    rounds = [(stream, hop) for hop in hops for stream in (out_scatter, gate_scatter)]
    own_columns = 2 * STATE // 4

    def column_copies(block):
        def copy(way, to):
            return remote(
                dbc_mine.at[block, pl.ds(pl.multiple_of(to * own_columns, own_columns), own_columns), :],
                dbc_there.at[way, block],
                bsend.at[way, block],
                brecv.at[way, block],
                tensor=to,
            )

        return copy(0, partner), copy(1, over), copy(2, diagonal)
    heads = bias_ref.shape[1]
    channels = inner_ref.shape[1]

    @pl.when(step == 0)
    def _():
        dstate[...] = jnp.zeros_like(dstate)
        dxbuf[Q:, :] = jnp.zeros((8, channels), F32)
        dbcbuf[Q:, :] = jnp.zeros((8, 2 * STATE), F32)
        grads_ref[...] = jnp.zeros_like(grads_ref)
        greet(True, True)
        for hop in hops + [0]:
            out_scatter.open(hop)
            gate_scatter.open(hop)
        branch.start()

    pl.when(step == 1)(lambda: branch.middle())
    early_rounds = {2: rounds[0], 4: rounds[1], 6: rounds[2]}
    for at_step, (stream, hop) in early_rounds.items():
        pl.when(step == at_step)(lambda: stream.round(hop))

    first = step == blocks - 1
    xbuf[0:8, :] = jnp.where(first, 0.0, prev_ref[...])
    bcbuf[0:8, :] = jnp.where(first, 0.0, sprev_ref[:, : 2 * STATE])
    xbuf[8:, :] = inner_ref[...]
    bcbuf[8:, :] = small_ref[:, : 2 * STATE]
    row, col = tri_masks()
    causal = row >= col
    causal_t = col >= row
    low_half = col < WIDTH
    pre_bc = conv_block(bcbuf, bcw_ref[...], bcb_ref[...])
    sig_bc = jax.nn.sigmoid(pre_bc)
    bc = low(pre_bc * sig_bc)
    b, c = bc[:, :STATE], bc[:, STATE:]
    raw = small_ref[:, 2 * STATE :] + bias_ref[...]
    dt = softplus(raw)
    a = -jnp.exp(alog_ref[...])
    cum = dot(causal.astype(F32), dt * a, precision=HIGHEST)
    cum_t = cum.T
    scores_t = dot(b, c, ((1,), (1,)))
    dstate_low = low(dstate[...])
    state_low = low(state_ref[0])
    carried[...] = dot(c, state_low)
    back[...] = dot(b, dstate_low)
    xw, xb = xw_ref[...], xb_ref[...]
    skip = skip_ref[...]
    dscores_t = jnp.zeros((Q, Q), F32)
    cols = jnp.zeros((Q, heads), F32)
    hot_row = lax.broadcasted_iota(jnp.int32, (2 * Q, heads), 0) // Q
    hot_col = lax.broadcasted_iota(jnp.int32, (2 * Q, heads), 1)
    for pair in range(heads // 2):
        sl = slice(2 * WIDTH * pair, 2 * WIDTH * (pair + 1))
        shifted = [xbuf[pl.ds(5 + k, Q), sl] for k in range(4)]
        pre = xb[:, sl] + xw[0:1, sl] * shifted[0]
        for k in range(1, 4):
            pre = pre + xw[k : k + 1, sl] * shifted[k]
        sig = jax.nn.sigmoid(pre)
        x = pre * sig
        _, _, dt_e = spread(dt, pair, low_half)
        _, _, skip_e = spread(skip, pair, low_half)
        cum_0, cum_1, cum_e = spread(cum, pair, low_half)
        last = cum_e[Q - 1 : Q, :]
        xh = x * dt_e
        xl = low(xh)
        gy = gy_ref[:, sl]
        gl = low(gy)
        zero = jnp.zeros_like(gl)
        g_stack = jnp.concatenate([jnp.where(low_half, gl, zero), jnp.where(low_half, zero, gl)], 0)
        dmixed_t = dot(xl, g_stack, ((1,), (1,)))
        mixes, zs = [], []
        for i, (h, cum_h) in enumerate(((2 * pair, cum_0), (2 * pair + 1, cum_1))):
            gap = cum_t[h : h + 1, :] - cum_h
            within = jnp.exp(jnp.where(causal_t, gap, NEG))
            mix = within * scores_t
            dm = dmixed_t[:, i * Q : (i + 1) * Q]
            dscores_t = dscores_t + dm * within
            z = low(dm * mix)
            zs.append(z)
            mixes.append(low(mix))
            rows_buf[h : h + 1, :] = jnp.sum(z.astype(F32), axis=0, keepdims=True)
        hot = (hot_col == hot_row + 2 * pair).astype(BF16)
        cols = cols + dot(jnp.concatenate(zs, 1), hot)
        dxh = dot(jnp.concatenate(mixes, 1), g_stack)
        to_end = jnp.exp(last - cum_e)
        from_state = to_end * back[:, sl]
        dxh = dxh + from_state
        grown = jnp.exp(cum_e) * gy
        cgy[:, sl] = low(grown)
        weighted[:, sl] = low(xh * to_end)
        sums[0:Q, sl] = low(grown * carried[:, sl])
        sums[Q : 2 * Q, sl] = low(xh * from_state)
        sums[2 * Q : 3 * Q, sl] = low(dxh * x)
        sums[3 * Q : 4 * Q, sl] = low(gy * x)
        decay_row[:, sl] = jnp.exp(last)
        dx = dxh * dt_e + skip_e * gy
        dpre = dx * (sig * (1.0 + pre * (1.0 - sig)))
        dxbuf[0:Q, sl] = dpre
        out = xw[3:4, sl] * dpre
        for k in range(3):
            out = out + xw[k : k + 1, sl] * dxbuf[pl.ds(3 - k, Q), sl]
        dinner_ref[:, sl] = low(out)
        for k in range(4):
            grads_ref[8 + k : 9 + k, sl] += jnp.sum(dpre * shifted[k], axis=0, keepdims=True)
        grads_ref[12:13, sl] += jnp.sum(dpre, axis=0, keepdims=True)
    head_of = lax.broadcasted_iota(jnp.int32, (channels, heads), 0) // WIDTH
    head = lax.broadcasted_iota(jnp.int32, (channels, heads), 1)
    head_hot = (head_of == head).astype(BF16)
    head_sums = dot(sums[...], head_hot)
    v, u = head_sums[0:Q], head_sums[Q : 2 * Q]
    t_x, t_skip = head_sums[2 * Q : 3 * Q], head_sums[3 * Q :]
    kept = jnp.sum(dstate[...] * state_ref[0], axis=0, keepdims=True) * decay_row[...]
    dlast = dot(jnp.broadcast_to(kept, (8, channels)), head_hot.astype(F32), precision=HIGHEST)[0:1]
    dlast = dlast + jnp.sum(u, axis=0, keepdims=True)
    dcum = rows_buf[0:heads, :].T - cols + v - u
    ddecay = dot(causal_t.astype(F32), dcum, precision=HIGHEST) + dlast
    ddt = (ddecay * a + t_x) * jax.nn.sigmoid(raw)
    ddt_ref[...] = low(ddt)
    grads_ref[4:5, 0:heads] += jnp.sum(ddt, axis=0, keepdims=True)
    grads_ref[5:6, 0:heads] += jnp.sum(ddecay * dt, axis=0, keepdims=True) * a
    grads_ref[6:7, 0:heads] += jnp.sum(t_skip, axis=0, keepdims=True)
    dsl = low(dscores_t)
    dc = dot(dsl, b, ((0,), (0,))) + dot(cgy[...], state_low, ((1,), (1,)))
    db = dot(dsl, c) + dot(weighted[...], dstate_low, ((1,), (1,)))
    dstate[...] = dstate[...] * decay_row[...] + dot(c.T, cgy[...])
    dbc = jnp.concatenate([db, dc], 1)
    dpre = dbc * (sig_bc * (1.0 + pre_bc * (1.0 - sig_bc)))
    dbcbuf[0:Q, :] = dpre
    bcw = bcw_ref[...]
    out = bcw[3:4] * dpre
    for k in range(3):
        out = out + bcw[k : k + 1] * dbcbuf[pl.ds(3 - k, Q), :]
    block = blocks - 1 - step
    dbc_mine[block] = low(out.T)
    for copy in column_copies(block):
        copy.start()
    for k in range(4):
        part = jnp.sum(dpre * bcbuf[pl.ds(5 + k, Q), :], axis=0, keepdims=True)
        at = 2 * STATE * (k % 3)
        grads_ref[2 + k // 3 : 3 + k // 3, at : at + 2 * STATE] += part
    grads_ref[3:4, 2 * STATE : 4 * STATE] += jnp.sum(dpre, axis=0, keepdims=True)
    dxbuf[Q:, :] = dxbuf[0:8, :]
    dbcbuf[Q:, :] = dbcbuf[0:8, :]

    @pl.when(step == blocks - 1)
    def _():
        for i in range(dbc_mine.shape[0]):
            for copy in column_copies(i):
                copy.wait_recv()
            mine = dbc_mine[i, pl.ds(pl.multiple_of(me * own_columns, own_columns), own_columns), :]
            total = mine.astype(F32)
            for way in range(3):
                total = total + dbc_there[way, i].astype(F32)
            dbc_ref[:, i * Q : (i + 1) * Q] = low(total)
        branch.finish()
        for stream, hop in rounds[3:]:
            stream.round(hop)
        out_scatter.finish()
        gate_scatter.finish()
        for i in range(dbc_mine.shape[0]):
            for copy in column_copies(i):
                copy.wait_send()


def mixer_backward(inner, small, gy, states, xw, xb, bcw, bcb, bias, alog, skip, gate_grad, out_grad, branch):
    n, share, side = gate_grad.shape
    tokens, features = branch.shape[1:]
    far = pl.BlockSpec(memory_space=pl.ANY)
    rows, channels = inner.shape
    blocks = rows // Q
    wide = small.shape[1]
    heads = bias.shape[1]
    at = lambda i: blocks - 1 - i
    before = lambda i: jnp.maximum(at(i) * (Q // 8) - 1, 0)
    return pl.pallas_call(
        backward_kernel,
        name="mixer_backward",
        grid=(blocks,),
        in_specs=[
            pl.BlockSpec((Q, channels), lambda i: (at(i), 0)),
            pl.BlockSpec((8, channels), lambda i: (before(i), 0)),
            pl.BlockSpec((Q, wide), lambda i: (at(i), 0)),
            pl.BlockSpec((8, wide), lambda i: (before(i), 0)),
            pl.BlockSpec((Q, channels), lambda i: (at(i), 0)),
            pl.BlockSpec((1, STATE, channels), lambda i: (at(i), 0, 0)),
            full(xw.shape), full(xb.shape), full(bcw.shape), full(bcb.shape),
            full(bias.shape), full(alog.shape), full(skip.shape),
            far, far, far,
        ],
        out_specs=[
            pl.BlockSpec((Q, channels), lambda i: (at(i), 0)),
            pl.BlockSpec((Q, heads), lambda i: (at(i), 0)),
            full((2 * STATE // 4, rows)),
            full((16, channels)), full((share, side)), full((share, side)), full((tokens, features)),
        ],
        out_shape=[
            jax.ShapeDtypeStruct((rows, channels), BF16),
            jax.ShapeDtypeStruct((rows, heads), BF16),
            jax.ShapeDtypeStruct((2 * STATE // 4, rows), BF16),
            jax.ShapeDtypeStruct((16, channels), F32),
            jax.ShapeDtypeStruct((share, side), F32),
            jax.ShapeDtypeStruct((share, side), F32),
            jax.ShapeDtypeStruct((tokens, features), F32),
        ],
        scratch_shapes=[
            pltpu.VMEM((Q + 8, channels), F32),
            pltpu.VMEM((Q + 8, 2 * STATE), F32),
            pltpu.VMEM((Q + 8, channels), F32),
            pltpu.VMEM((Q + 8, 2 * STATE), F32),
            pltpu.VMEM((STATE, channels), F32),
            pltpu.VMEM((Q, channels), F32),
            pltpu.VMEM((Q, channels), F32),
            pltpu.VMEM((16, Q), F32),
            pltpu.VMEM((4 * Q, channels), BF16),
            pltpu.VMEM((Q, channels), BF16),
            pltpu.VMEM((Q, channels), BF16),
            pltpu.VMEM((1, channels), F32),
            pltpu.VMEM((blocks, 2 * STATE, Q), BF16),
            pltpu.VMEM((3, blocks, 2 * STATE // 4, Q), BF16),
            pltpu.SemaphoreType.DMA((3, blocks)),
            pltpu.SemaphoreType.DMA((3, blocks)),
        ]
        + line_scatter_scratch(n, share, side)
        + line_scatter_scratch(n, share, side)
        + quad_scatter_scratch(tokens, features),
        compiler_params=pltpu.CompilerParams(collective_id=2, has_side_effects=True),
        cost_estimate=pl.CostEstimate(
            flops=rows * channels * Q * 20, bytes_accessed=rows * channels * 20, transcendentals=rows * channels * 10
        ),
    )(inner, inner, small, small, gy, states, xw, xb, bcw, bcb, bias, alog, skip, gate_grad, out_grad, branch)


def remote(src, dst, send, recv, **to):
    return pltpu.make_async_remote_copy(
        src_ref=src, dst_ref=dst, send_sem=send, recv_sem=recv, device_id=to, device_id_type=MESH
    )


def line_place():
    me = lax.axis_index("dp")
    return me // 2, me % 2, lax.axis_size("dp") // 2


def quad_place():
    me = lax.axis_index("tensor")
    x, core = me // 2, me % 2
    return me, x * 2 + 1 - core, (1 - x) * 2 + core, (1 - x) * 2 + 1 - core


def greet(line, quad):
    barrier = pltpu.get_barrier_semaphore()
    count = 0
    if line:
        z, y, nz = line_place()
        pl.semaphore_signal(barrier, inc=1, device_id={"dp": z * 2 + 1 - y}, device_id_type=MESH)
        count = 1

        @pl.when(z > 0)
        def _():
            pl.semaphore_signal(barrier, inc=1, device_id={"dp": z * 2 - 2 + y}, device_id_type=MESH)

        @pl.when(z < nz - 1)
        def _():
            pl.semaphore_signal(barrier, inc=1, device_id={"dp": z * 2 + 2 + y}, device_id_type=MESH)

        count = count + jnp.where(z > 0, 1, 0) + jnp.where(z < nz - 1, 1, 0)
    if quad:
        for other in quad_place()[1:]:
            pl.semaphore_signal(barrier, inc=1, device_id={"tensor": other}, device_id_type=MESH)
        count = count + 3
    pl.semaphore_wait(barrier, count)


class LineGather:
    def __init__(self, own, out, send, recv, local):
        self.own, self.out, self.send, self.recv = own, out, send, recv
        self.z, self.y, self.nz = line_place()
        self.local = pltpu.make_async_copy(own, out.at[self.z * 2 + self.y], local)

    def copy(self, z, y, way, src=None):
        slot = z * 2 + y
        to = (self.z * 2 + 2 + self.y, self.z * 2 - 2 + self.y, self.z * 2 + 1 - self.y)[way]
        return remote(
            self.out.at[slot] if src is None else src,
            self.out.at[slot],
            self.send.at[slot, way],
            self.recv.at[slot],
            dp=to,
        )

    def each(self, act):
        z, y, nz = self.z, self.y, self.nz
        pl.when(z < nz - 1)(lambda: act(self.copy(z, y, 0, self.own)))
        pl.when(z > 0)(lambda: act(self.copy(z, y, 1, self.own)))
        act(self.copy(z, y, 2, self.own))

    def start(self):
        self.each(lambda c: c.start())
        self.local.start()

    def relay(self, hop):
        z, y, nz = self.z, self.y, self.nz

        @pl.when(z >= hop)
        def _():
            self.copy(z - hop, y, 2).wait_recv()
            pl.when(z < nz - 1)(lambda: self.copy(z - hop, y, 0).start())
            self.copy(z - hop, y, 2).start()

        @pl.when(z + hop < nz)
        def _():
            self.copy(z + hop, y, 2).wait_recv()
            pl.when(z > 0)(lambda: self.copy(z + hop, y, 1).start())
            self.copy(z + hop, y, 2).start()

    def finish(self):
        z, y, nz = self.z, self.y, self.nz
        for other in range(nz):
            self.copy(other, 1 - y, 2).wait_recv()
        self.local.wait()
        self.each(lambda c: c.wait_send())
        for hop in range(1, nz):

            @pl.when(z >= hop)
            def _():
                pl.when(z < nz - 1)(lambda: self.copy(z - hop, y, 0).wait_send())
                self.copy(z - hop, y, 2).wait_send()

            @pl.when(z + hop < nz)
            def _():
                pl.when(z > 0)(lambda: self.copy(z + hop, y, 1).wait_send())
                self.copy(z + hop, y, 2).wait_send()


class QuadGather:
    def __init__(self, own, out, send, recv, local):
        self.own, self.out, self.send, self.recv = own, out, send, recv
        self.me, self.partner, self.over, self.diagonal = quad_place()
        self.local = pltpu.make_async_copy(own, out.at[self.me], local)

    def copy(self, slot, src, way, to):
        return remote(src, self.out.at[slot], self.send.at[way], self.recv.at[slot], tensor=to)

    def sends(self):
        return (
            self.copy(self.me, self.own, 0, self.over),
            self.copy(self.me, self.own, 1, self.partner),
            self.copy(self.over, self.out.at[self.over], 2, self.partner),
        )

    def arrival(self, slot):
        return self.copy(slot, self.own, 0, self.partner)

    def start(self):
        across, beside, _ = self.sends()
        across.start()
        beside.start()
        self.local.start()

    def relay(self):
        self.arrival(self.over).wait_recv()
        self.sends()[2].start()

    def finish(self):
        self.arrival(self.partner).wait_recv()
        self.arrival(self.diagonal).wait_recv()
        self.local.wait()
        for send in self.sends():
            send.wait_send()


def line_semaphores(n):
    return [
        pltpu.SemaphoreType.DMA((n, 3)),
        pltpu.SemaphoreType.DMA((n,)),
        pltpu.SemaphoreType.DMA,
    ]


def quad_semaphores():
    return [
        pltpu.SemaphoreType.DMA((3,)),
        pltpu.SemaphoreType.DMA((4,)),
        pltpu.SemaphoreType.DMA,
    ]


def first_kernel(pack_ref, rows_ref, all_ref, tokens_ref, ls, lr, ll, qs, qr, ql):
    greet(True, True)
    line = LineGather(pack_ref, all_ref, ls, lr, ll)
    quad = QuadGather(rows_ref, tokens_ref, qs, qr, ql)
    line.start()
    quad.start()
    for hop in range(1, line.nz):
        line.relay(hop)
        if hop == 1:
            quad.relay()
    quad.finish()
    line.finish()


def gather_first(pack, rows):
    n = lax.axis_size("dp")
    whole = pl.BlockSpec(memory_space=pltpu.VMEM)
    far = pl.BlockSpec(memory_space=pl.ANY)
    return pl.pallas_call(
        first_kernel,
        name="gather_first",
        in_specs=[whole, whole],
        out_specs=[far, far],
        out_shape=[
            jax.ShapeDtypeStruct((n,) + pack.shape, pack.dtype),
            jax.ShapeDtypeStruct((4,) + rows.shape, rows.dtype),
        ],
        scratch_shapes=line_semaphores(n) + quad_semaphores(),
        compiler_params=pltpu.CompilerParams(collective_id=0, has_side_effects=True),
    )(pack, rows)


def add_rows(target, *sources):
    rows = target.shape[0]
    group = 48 if rows % 48 == 0 else 32

    @pl.loop(0, rows // group)
    def _(i):
        at = pl.ds(pl.multiple_of(i * group, 16), group)
        total = sources[0][at, :].astype(F32)
        for source in sources[1:]:
            total = total + source[at, :].astype(F32)
        target[at, :] = total.astype(target.dtype)


class LineScatter:
    def __init__(self, src, out, mine, near, below, above, sems):
        self.src, self.out, self.mine, self.near = src, out, mine, near
        self.below, self.above, self.sems = below, above, sems
        self.z, self.y, self.nz = line_place()

    def load(self, t):
        return pltpu.make_async_copy(
            self.src.at[t * 2 + self.y], self.mine.at[t], self.sems.at[0, t]
        )

    def beside(self, t):
        other = 1 - self.y
        return remote(
            self.src.at[t * 2 + other], self.near.at[t], self.sems.at[1, t], self.sems.at[2, t],
            dp=self.z * 2 + other,
        )

    def up(self, t):
        return remote(
            self.near.at[t], self.below.at[t], self.sems.at[3, t], self.sems.at[4, t],
            dp=self.z * 2 + 2 + self.y,
        )

    def down(self, t):
        return remote(
            self.near.at[t], self.above.at[t], self.sems.at[3, t], self.sems.at[5, t],
            dp=self.z * 2 - 2 + self.y,
        )

    def open(self, hop):
        z, nz = self.z, self.nz

        def begin(t):
            self.beside(t).start()
            self.load(t).start()

        if hop == 0:
            begin(z)
        else:
            pl.when(z + hop < nz)(lambda: begin(z + hop))
            pl.when(z >= hop)(lambda: begin(z - hop))

    def round(self, hop):
        z, nz = self.z, self.nz

        def ready(t):
            self.load(t).wait()
            self.beside(t).wait_recv()

        @pl.when(z + hop < nz)
        def _():
            t = z + hop
            ready(t)

            @pl.when(z > 0)
            def _():
                self.up(t).wait_recv()
                add_rows(self.near.at[t], self.mine.at[t], self.near.at[t], self.below.at[t])

            @pl.when(z == 0)
            def _():
                add_rows(self.near.at[t], self.mine.at[t], self.near.at[t])

            self.up(t).start()

        @pl.when(z >= hop)
        def _():
            t = z - hop
            ready(t)

            @pl.when(z < nz - 1)
            def _():
                self.down(t).wait_recv()
                add_rows(self.near.at[t], self.mine.at[t], self.near.at[t], self.above.at[t])

            @pl.when(z == nz - 1)
            def _():
                add_rows(self.near.at[t], self.mine.at[t], self.near.at[t])

            self.down(t).start()

    def finish(self):
        z, nz = self.z, self.nz
        self.load(z).wait()
        self.beside(z).wait_recv()
        pl.when(z > 0)(lambda: self.up(z).wait_recv())
        pl.when(z < nz - 1)(lambda: self.down(z).wait_recv())
        own = (self.mine.at[z], self.near.at[z])

        @pl.when(z == 0)
        def _():
            add_rows(self.out, *own, self.above.at[z])

        @pl.when(z == nz - 1)
        def _():
            add_rows(self.out, *own, self.below.at[z])

        @pl.when((z > 0) & (z < nz - 1))
        def _():
            add_rows(self.out, *own, self.below.at[z], self.above.at[z])

        for t in range(nz):
            self.beside(t).wait_send()
            pl.when(z < t)(lambda: self.up(t).wait_send())
            pl.when(z > t)(lambda: self.down(t).wait_send())


class QuadScatter:
    def __init__(self, src, out, mine, side, far, sems):
        self.src, self.out, self.mine, self.side, self.far = src, out, mine, side, far
        self.sems = sems
        self.me, self.partner, self.over, self.diagonal = quad_place()

    def copies(self):
        return (
            pltpu.make_async_copy(self.src.at[self.me], self.mine.at[0], self.sems.at[0]),
            pltpu.make_async_copy(self.src.at[self.over], self.mine.at[1], self.sems.at[1]),
            remote(
                self.src.at[self.diagonal], self.side.at[1], self.sems.at[2], self.sems.at[3],
                tensor=self.partner,
            ),
            remote(
                self.src.at[self.partner], self.side.at[0], self.sems.at[4], self.sems.at[5],
                tensor=self.partner,
            ),
            remote(self.side.at[1], self.far, self.sems.at[6], self.sems.at[7], tensor=self.over),
        )

    def start(self):
        own, passing, first, second, _ = self.copies()
        first.start()
        passing.start()
        second.start()
        own.start()

    def middle(self):
        _, passing, first, _, across = self.copies()
        passing.wait()
        first.wait_recv()
        add_rows(self.side.at[1], self.mine.at[1], self.side.at[1])
        across.start()

    def finish(self):
        own, _, first, second, across = self.copies()
        own.wait()
        second.wait_recv()
        across.wait_recv()
        if self.out is not None:
            add_rows(self.out, self.mine.at[0], self.side.at[0], self.far)
        first.wait_send()
        second.wait_send()
        across.wait_send()


def line_scatter_scratch(n, rows, columns):
    return [pltpu.VMEM((n // 2, rows, columns), BF16)] * 4 + [pltpu.SemaphoreType.DMA((6, n // 2))]


def quad_scatter_scratch(rows, columns):
    return [
        pltpu.VMEM((2, rows, columns), BF16),
        pltpu.VMEM((2, rows, columns), BF16),
        pltpu.VMEM((rows, columns), BF16),
        pltpu.SemaphoreType.DMA((8,)),
    ]


def last_kernel(
    small_ref, one_ref, two_ref, dx_ref, hidden_ref, dout_ref, gain_ref, mix_ref, scale_ref,
    d_hidden_ref, bc_ref, dt_ref, left_ref, right_ref, flat_ref, shared_ref,
    *scratch,
):
    s0, s1, s2 = scratch[0:5], scratch[5:10], scratch[10:15]
    quad_scratch = scratch[15:19]
    flat, flat_all, shared_own, shared_all, small_sum, bc_all = scratch[19:25]
    ls, lr, ll, qs, qr, ql, bs, br, bl = scratch[25:34]
    greet(True, True)
    small = LineScatter(small_ref, small_sum, *s0)
    one = LineScatter(one_ref, left_ref, *s1)
    two = LineScatter(two_ref, right_ref, *s2)
    dx = QuadScatter(dx_ref, None, *quad_scratch)
    hops = list(range(one.nz - 1, 0, -1))
    for hop in hops + [0]:
        small.open(hop)
    dx.start()
    for hop in hops + [0]:
        one.open(hop)
        two.open(hop)
    dx.middle()
    for hop in hops:
        small.round(hop)
    small.finish()
    width = small_sum.shape[1]
    columns = QuadGather(small_sum, bc_all, bs, br, bl)
    columns.start()
    middle = max(len(hops) - 1, 1)
    for i, hop in enumerate(hops):
        one.round(hop)
        two.round(hop)
        if i == 0:
            columns.relay()
    dx.finish()
    mine, side, far = quad_scratch[0].at[0], quad_scratch[1].at[0], quad_scratch[2]
    flat[...] = mix_ref[...]
    flat[7:8, :] = scale_ref[...]
    half = flat.shape[1]
    features = hidden_ref.shape[1]
    group = 32

    def token_rows(i, total):
        at = pl.ds(pl.multiple_of(i * group, group), group)
        d_normed = mine[at, :].astype(F32) + side[at, :].astype(F32) + far[at, :].astype(F32)
        hidden = hidden_ref[at, :].astype(F32)
        rh = lax.rsqrt(jnp.mean(hidden * hidden, axis=-1, keepdims=True) + EPSILON)
        weighted = d_normed * gain_ref[...]
        inner_sum = jnp.sum(weighted * hidden, axis=-1, keepdims=True) / features
        d_hidden_ref[at, :] = (
            dout_ref[at, :].astype(F32) + rh * weighted - hidden * (rh * rh * rh) * inner_sum
        )
        return total + jnp.sum(d_normed * hidden * rh, axis=0, keepdims=True)

    gain = lax.fori_loop(
        0, hidden_ref.shape[0] // group, token_rows, jnp.zeros((1, features), F32)
    )
    flat[0:1, :] = gain[:, :half]
    flat[1:2, :] = gain[:, half:]
    gather = LineGather(flat, flat_all, ls, lr, ll)
    gather.start()
    for hop in range(1, gather.nz):
        gather.relay(hop)
    gather.finish()
    total = flat_all[0]
    for i in range(1, flat_all.shape[0]):
        total = total + flat_all[i]
    flat_ref[...] = total
    shared_own[...] = total[0:8, :]
    shared = QuadGather(shared_own, shared_all, qs, qr, ql)
    shared.start()
    one.finish()
    shared.relay()
    two.finish()
    columns.finish()
    shared.finish()
    shared_ref[...] = shared_all[0] + shared_all[1] + shared_all[2] + shared_all[3]
    own_columns = bc_ref.shape[1] // 4
    for t in range(4):
        bc_ref[:, t * own_columns : (t + 1) * own_columns] = bc_all[t, :, :own_columns]
    dt_ref[...] = small_sum[:, own_columns : own_columns + dt_ref.shape[1]]


def last_exchange(small, one, two, dx, hidden, d_out, gain, mix, scale, heads):
    n, rows, width = small.shape
    side = one.shape[2]
    tokens, features = hidden.shape
    half = mix.shape[1]
    far = pl.BlockSpec(memory_space=pl.ANY)
    near = pl.BlockSpec(memory_space=pltpu.VMEM)
    shape = jax.ShapeDtypeStruct
    return pl.pallas_call(
        last_kernel,
        name="last_exchange",
        in_specs=[far] * 4 + [near] * 5,
        out_specs=[near] * 7,
        out_shape=[
            shape((tokens, features), F32),
            shape((rows, 2 * STATE), F32),
            shape((rows, heads), F32),
            shape((rows, side), F32),
            shape((rows, side), F32),
            shape(mix.shape, F32),
            shape((8, half), F32),
        ],
        scratch_shapes=line_scatter_scratch(n, rows, width)
        + line_scatter_scratch(n, rows, side)
        + line_scatter_scratch(n, rows, side)
        + quad_scatter_scratch(tokens, features)
        + [
            pltpu.VMEM(mix.shape, F32),
            pltpu.VMEM((n,) + mix.shape, F32),
            pltpu.VMEM((8, half), F32),
            pltpu.VMEM((4, 8, half), F32),
            pltpu.VMEM((rows, width), F32),
            pltpu.VMEM((4, rows, width), F32),
        ]
        + line_semaphores(n)
        + quad_semaphores()
        + quad_semaphores(),
        compiler_params=pltpu.CompilerParams(collective_id=3, has_side_effects=True),
    )(small, one, two, dx, hidden, d_out, gain, mix, scale)


def local(
    hidden_in, d_out, in_gain, w_zx, w_dt, w_bc, w_out,
    conv_x_w, conv_x_b, conv_bc_w, conv_bc_b, dt_bias, a_log, d_skip, norm_scale,
):
    _, rows_local, width = hidden_in.shape
    inner_local = w_zx.shape[2]
    heads = w_dt.shape[1]
    tensor_index = lax.axis_index("tensor")
    parts = lax.axis_size("tensor")
    own_width = in_gain.shape[0]
    spare = jnp.zeros((own_width, 127 - heads), BF16)
    first_pack = jnp.concatenate([w_zx[:, 1, :], w_bc, w_dt, in_gain[:, None], spare], 1)
    first, hidden_bf = gather_first(first_pack, hidden_in[0])
    first = first.reshape(width, -1)
    hidden_bf = hidden_bf.reshape(-1, width)
    second_pack = jnp.concatenate([w_zx[:, 0, :], w_out], 1)
    w_inner = first[:, :inner_local]
    w_small = first[:, inner_local : inner_local + 2 * STATE + heads]
    gain = first[:, inner_local + 2 * STATE + heads].astype(F32)[None]

    hidden = hidden_bf.astype(F32)
    rh = lax.rsqrt(jnp.mean(hidden * hidden, axis=-1, keepdims=True) + EPSILON)
    xn = low(hidden * rh * gain)
    inner = dot(xn, w_inner)
    small = dot(xn, w_small)
    params = (
        conv_x_w, conv_x_b[None], conv_bc_w, conv_bc_b[None], dt_bias[None], a_log[None], d_skip[None],
    )
    y, states, second, dout_all = mixer_forward(inner, small, *params, second_pack, d_out[0])
    second = second.reshape(width, -1)
    dout_all = dout_all.reshape(-1, width)
    w_gate, w_o = second[:, :inner_local], second[:, inner_local:]
    gate = dot(xn, w_gate)
    dyn = dot(dout_all, w_o)
    sig = jax.nn.sigmoid(gate)
    act = gate * sig
    gated = y * act
    scale = norm_scale[None]
    scaled = dyn * scale
    sums = lax.psum(jnp.stack([jnp.sum(gated * gated, -1), jnp.sum(scaled * gated, -1)]), "tensor")
    channels = inner_local * parts
    r = lax.rsqrt(sums[0] / channels + EPSILON)[:, None]
    yn = low(gated * r * scale)
    d_gated = r * scaled - gated * (r * r * r) * sums[1][:, None] / channels
    g_scale = jnp.sum(dyn * gated * r, axis=0)
    gy = d_gated * act
    d_gate = low(d_gated * y * (sig * (1.0 + gate * (1.0 - sig))))
    n = lax.axis_size("dp")
    g_out = low(dot(dout_all, yn, ((0,), (0,)))).reshape(n, own_width, -1)
    g_gate = low(dot(xn, d_gate, ((0,), (0,)))).reshape(n, own_width, -1)
    partial_out = low(dot(yn, w_o, ((1,), (1,)))).reshape(parts, rows_local, width)
    d_inner, d_dt, d_bc, mix, gate_sum, out_sum, branch = mixer_backward(
        inner, small, gy, states, *params, g_gate, g_out, partial_out
    )
    block_out = low(hidden_in[0].astype(F32) + branch)
    own_columns = 2 * STATE // parts
    spare = jnp.zeros((inner.shape[0], 128 - own_columns - heads), BF16)
    late_small = jnp.concatenate([d_bc.T, d_dt, spare], 1)
    half = inner_local // 2
    g_one = low(dot(xn, d_inner[:, :half], ((0,), (0,)))).reshape(n, own_width, -1)
    g_two = low(dot(xn, d_inner[:, half:], ((0,), (0,)))).reshape(n, own_width, -1)
    g_small = low(dot(xn, late_small, ((0,), (0,)))).reshape(n, own_width, -1)
    w_small_own = jnp.concatenate(
        [
            lax.dynamic_slice_in_dim(first, inner_local + tensor_index * own_columns, own_columns, 1),
            first[:, inner_local + 2 * STATE : inner_local + 2 * STATE + 128 - own_columns],
        ],
        1,
    )
    d_xn = dot(d_gate, w_gate, ((1,), (1,))) + dot(d_inner, w_inner, ((1,), (1,)))
    d_xn = low(d_xn + dot(late_small, w_small_own, ((1,), (1,)))).reshape(parts, rows_local, width)
    d_hidden, g_w_bc, g_w_dt, left, right, flat, shared = last_exchange(
        g_small, g_one, g_two, d_xn, hidden_in[0], d_out[0], gain, mix, g_scale[None], heads
    )
    own = lax.dynamic_slice_in_dim(
        shared[:2].reshape(-1), lax.axis_index("dp") * own_width, own_width, 0
    )
    g_bc = shared[2:4].reshape(-1)[: 5 * 2 * STATE].reshape(5, 2 * STATE)
    g_x = flat[8:13]
    g_zx = jnp.stack([gate_sum, jnp.concatenate([left, right], 1)], 1)
    return (
        block_out[None],
        d_hidden[None],
        own,
        g_zx,
        g_w_dt,
        g_w_bc,
        out_sum,
        g_x[:4],
        g_x[4],
        g_bc[:4],
        g_bc[4],
        flat[4, :heads],
        flat[5, :heads],
        flat[6, :heads],
        flat[7],
    )


def solution(mesh):
    tokens = P("dp", "tensor", None)
    specs = (
        tokens,
        tokens,
        P("dp"),
        P("dp", None, "tensor"),
        P("dp", "tensor"),
        P("dp", None),
        P("dp", "tensor"),
        P(None, "tensor"),
        P("tensor"),
        P(),
        P(),
        P("tensor"),
        P("tensor"),
        P("tensor"),
        P("tensor"),
    )
    return jax.shard_map(local, mesh=mesh, in_specs=specs, out_specs=specs, check_vma=False)
```
